128 devices in a mesh: sub: 16 (over x_hi, z, core), sta: 8 (over x_lo, y).
Axes of the slice: x: 4 (x_hi: 2, x_lo: 2; x = x_hi * 2 + x_lo), y: 4, z: 4, core: 2. Of those that a mesh axis runs over, the one named last changes fastest.
Arguments:
- voltages: bfloat16 [16, 2, 64, 65536], P('sub', None, 'sta'), may hold values from -6 to 6
- beam_weights: bfloat16 [16, 2, 32, 64], P('sub'), may hold values from -0.5 to 0.5
- station_delays: int32 [64], P('sta'), may hold values from 0 to 16383
- dm_index: int32 [32, 1], P('sta'), may hold values from 1 to 8
Outputs:
- dedispersed: float32 [16, 2, 32, 1, 65536], P(None, None, None, None, ('sub', 'sta'))
- intensity: float32 [32, 1, 65536], P(None, None, ('sub', 'sta'))
The draws below stay inside these ranges and needn't reach their ends.
Inputs may be any that keep to these rules, and one draw needn't show every extreme that they name: `station_delays`: delays in whole samples. `dm_index`: dispersion measure in steps of 10.
All inputs are finite; a program needn't handle non-finite values.
Results may differ from the reference program's by a relative error of at most 0.0006.
Values may be sent and summed in bfloat16 or wider, within the bound.
No kernel may reach another device: no remote copies, remote signals or barrier semaphores. Data moves between devices by JAX's collectives and lax.ppermute only.
A program may use at most 320 MiB of HBM per device.

```python
import jax
import jax.numpy as jnp
from jax import lax

STATIONS = 64
BEAMS = 32
DMS = 1
SAMPLES = 65536
SUBBANDS = 16


def set_ends(values, key, low, largest):
    extent = values.shape
    spot = [jax.random.randint(jax.random.fold_in(key, axis), (), 0, extent[axis]) for axis in range(len(extent))]
    values = values.at[tuple(spot)].set(low)
    longest = extent.index(max(extent))
    spot[longest] = (spot[longest] + 1) % extent[longest]
    return values.at[tuple(spot)].set(largest)


def block_scale(rng, shape, split, low, top_value):
    def one(axis_at, shards_of):
        heights = jax.random.uniform(jax.random.fold_in(jax.random.fold_in(rng, 6), axis_at), (shards_of,), jnp.float32, low / len(split), top_value / len(split))
        return jnp.repeat(jnp.exp(heights), shape[axis_at] // shards_of).reshape((-1,) + (1,) * (len(shape) - axis_at - 1))

    gain = one(*split[0])
    for cut in split[1:]:
        gain = gain * one(*cut)
    return gain


def bell_draw(own_key, dims, scale, limit, pieces=(), kind=jnp.bfloat16):
    drawn = jax.random.normal(own_key, dims, jnp.float32) * scale
    if len(pieces) > 0:
        drawn = block_scale(own_key, dims, pieces, -0.22, 0.18) * drawn
    return jnp.clip(drawn, min=-limit, max=limit).astype(kind)


def setup_inputs(seed: int = 0) -> dict:
    streams_of = jax.random.split(jax.random.key(seed), 5)
    voltages = bell_draw(streams_of[0], (SUBBANDS, 2, STATIONS, SAMPLES), 1.0, 6.0, ((0, 16), (2, 8)))
    beam_weights = bell_draw(streams_of[1], (SUBBANDS, 2, BEAMS, STATIONS), (2 * STATIONS) ** -0.5, 0.5, ((0, 16),))
    station_delays = set_ends(jax.random.randint(streams_of[2], (STATIONS,), 0, SAMPLES // 4), jax.random.fold_in(streams_of[2], 1), 0, (SAMPLES // 4) - 1).astype(jnp.int32)
    dm_index = set_ends(jax.random.randint(streams_of[3], (BEAMS, DMS), 1, 9), jax.random.fold_in(streams_of[3], 1), 1, 8).astype(jnp.int32)
    return dict(voltages=voltages, beam_weights=beam_weights, station_delays=station_delays, dm_index=dm_index)


TWO_PI = 6.283185307179586
DISPERSION = 4148808000.0
DM_STEP = 10.0
BASE_FREQ = 120.0
CHANNEL_WIDTH = 0.1953125


def chirp_base(subband, total_len):
    positions = jnp.arange(total_len, dtype=jnp.int32)
    signed_bin = jnp.where(positions < total_len // 2, positions, positions - total_len)
    offset = CHANNEL_WIDTH * signed_bin.astype(jnp.float32) / total_len
    centre = BASE_FREQ + CHANNEL_WIDTH * (subband.astype(jnp.float32) + 0.5)
    return TWO_PI * DISPERSION * offset * offset / (centre * centre * (centre + offset))


def reference(voltages, beam_weights, station_delays, dm_index):
    dm_value = DM_STEP * dm_index.astype(jnp.float32)

    def one_subband(inputs):
        subband, volts, weights = inputs
        shifted = jax.vmap(lambda rows, shift_by: jnp.roll(rows, shift_by, axis=-1), in_axes=(1, 0), out_axes=1)(volts, station_delays)
        real_part = jnp.dot(weights[0], shifted[0], preferred_element_type=jnp.float32) - jnp.dot(weights[1], shifted[1], preferred_element_type=jnp.float32)
        imag_part = jnp.dot(weights[0], shifted[1], preferred_element_type=jnp.float32) + jnp.dot(weights[1], shifted[0], preferred_element_type=jnp.float32)
        spectrum = jnp.fft.fft(lax.complex(real_part, imag_part), axis=-1)
        phase_table = dm_value[:, :, None] * chirp_base(subband, SAMPLES)[None, None, :]
        chirped = spectrum[:, None, :] * lax.complex(jnp.cos(phase_table), jnp.sin(phase_table))
        series = jnp.fft.ifft(chirped, axis=-1)
        return jnp.stack([jnp.real(series), jnp.imag(series)], axis=0)

    dedispersed = lax.map(one_subband, (jnp.arange(SUBBANDS, dtype=jnp.int32), voltages, beam_weights))
    intensity = jnp.mean(dedispersed[:, 0] * dedispersed[:, 0] + dedispersed[:, 1] * dedispersed[:, 1], axis=0)
    return dedispersed, intensity
```

```python
import functools

import jax
import jax.numpy as jnp
import numpy as np
from jax import lax
from jax.experimental import pallas as pl
from jax.experimental.pallas import tpu as pltpu
from jax.sharding import PartitionSpec as P

TWO_PI = 6.283185307179586
DISPERSION = 4148808000.0
DM_STEP = 10.0
BASE_FREQ = 120.0
CHANNEL_WIDTH = 0.1953125

TOTAL = 65536
ROOT = 256
HALF = 128
LANES = 128
STA = 8
BLOCK = TOTAL // STA
TILES = BLOCK // LANES
BEAMS = 4
DEVICES = 128
CODE_STEP = 64.0
LEVELS = 32767.0
FLOOR = 1e-33

f32 = jnp.float32
bf16 = jnp.bfloat16


def split_np(table):
    high = table.astype(bf16)
    low = (table - high.astype(np.float64)).astype(bf16)
    return high, low


@functools.lru_cache(maxsize=None)
def tables():
    m = np.arange(HALF)
    fwd = []
    for parity in range(2):
        angle = 2 * np.pi * (((2 * m[:, None] + parity) * m[None, :]) % ROOT) / ROOT
        c, s = np.cos(angle), np.sin(angle)
        fwd.append(np.block([[c, s], [-s, c]]))
    fwd = np.stack(fwd)
    bwd = fwd.transpose(0, 2, 1)
    order = (2 * np.arange(64)[None, :] + np.arange(2)[:, None]).reshape(-1)
    order = np.concatenate([order, HALF + order])
    last = bwd[:, order, :]

    def left(t):
        hi, lo = split_np(t)
        return np.concatenate([hi, hi, lo], axis=2)

    def right(t):
        hi, lo = split_np(t)
        return np.concatenate([hi, hi, lo], axis=1)

    rows = np.concatenate([2 * m, 2 * m + 1])
    angle = 2 * np.pi * (rows[:, None] * np.arange(ROOT)[None, :]) / TOTAL
    twiddle = np.stack([np.cos(angle), np.sin(angle)]).astype(np.float32)
    return left(fwd), right(bwd), right(fwd), left(last), twiddle


def code_of(peak):
    return jnp.ceil(jnp.log(jnp.maximum(peak, FLOOR)) * (CODE_STEP / 0.6931471805599453)) + 1.0


def scale_of(code):
    return jnp.exp2(code * (1.0 / CODE_STEP))


def quantize(x, inverse):
    return jnp.round(x * inverse).astype(jnp.int32).astype(jnp.int16)


def widen(q):
    return q.astype(jnp.int32).astype(f32)


def shift_kernel(delay_ref, v_ref, out_ref, merged_ref):
    lane = lax.broadcasted_iota(jnp.int32, (STA, LANES), 1)
    row = lax.broadcasted_iota(jnp.int32, (STA, LANES), 0)
    fine = jnp.zeros((STA, LANES), jnp.int32)
    for q in range(STA):
        fine = jnp.where(row == q, delay_ref[q] & (LANES - 1), fine)
    index = (lane - fine) & (LANES - 1)
    keep = lane >= fine
    count = TOTAL // LANES
    wrap = 128
    picks = [row == q for q in range(STA)]

    def turned(p, j):
        x = v_ref[0, p, :, pl.ds(pl.multiple_of(j * LANES, LANES), LANES)].astype(f32)
        return jnp.take_along_axis(x, index, axis=1)

    for p in range(2):
        unroll = 8

        def fill(i, before):
            for u in range(unroll):
                j = i * unroll + u
                now = turned(p, j)
                merged_ref[wrap + j] = jnp.where(keep, now, before)
                before = now
            return before

        lax.fori_loop(0, count // unroll, fill, turned(p, count - 1))

        def front(i, carry):
            for u in range(unroll):
                merged_ref[i * unroll + u] = merged_ref[count + i * unroll + u]
            return carry

        lax.fori_loop(0, wrap // unroll, front, 0)
        starts = [wrap - lax.shift_right_logical(delay_ref[q], 7) for q in range(STA)]

        def move(i, carry):
            parts = []
            for u in range(4):
                j = i * 4 + u
                x = merged_ref[starts[0] + j]
                for q in range(1, STA):
                    x = jnp.where(picks[q], merged_ref[starts[q] + j], x)
                parts.append(x)
            wide = jnp.concatenate(parts, axis=1).astype(bf16)
            d = i // (TILES // 4)
            at = (i % (TILES // 4)) * (4 * LANES)
            out_ref[d, p, :, pl.ds(pl.multiple_of(at, 4 * LANES), 4 * LANES)] = wide
            return carry

        lax.fori_loop(0, count // 4, move, 0)


def beam_kernel(v_ref, w_ref, out_ref, sums_ref):
    w = w_ref[0].astype(f32)
    rows = []
    for d in range(STA):
        w_re = w[0, d * BEAMS : (d + 1) * BEAMS]
        w_im = w[1, d * BEAMS : (d + 1) * BEAMS]
        rows.append(jnp.concatenate([w_re, -w_im], axis=1))
        rows.append(jnp.concatenate([w_im, w_re], axis=1))
    left = jnp.concatenate(rows, axis=0).astype(bf16)
    chunk = 1024

    def mix(i, peak):
        at = pl.ds(pl.multiple_of(i * chunk, chunk), chunk)
        volts = jnp.concatenate(
            [v_ref[g, 0, :, at] for g in range(STA)] + [v_ref[g, 1, :, at] for g in range(STA)], axis=0
        )
        sums = jnp.dot(left, volts, preferred_element_type=f32)
        sums_ref[:, at] = sums
        for u in range(chunk // LANES):
            peak = jnp.maximum(peak, jnp.abs(sums[:, u * LANES : (u + 1) * LANES]))
        return peak

    peak = lax.fori_loop(0, BLOCK // chunk, mix, jnp.zeros((64, LANES), f32))
    code = code_of(peak)
    inverse = LEVELS / scale_of(code)
    for d in range(STA):
        at8 = slice(d * 8, d * 8 + 8)
        factor = inverse[at8]
        out_ref[d, :, BLOCK:] = code[at8].astype(jnp.int32).astype(jnp.int16)

        def pack(i, carry):
            at = pl.multiple_of(i * 1024, 1024)
            x = sums_ref[at8, pl.ds(at, 1024)]
            x = x * jnp.concatenate([factor] * 8, axis=1)
            out_ref[d, :, pl.ds(at, 1024)] = jnp.round(x).astype(jnp.int32).astype(jnp.int16)
            return carry

        lax.fori_loop(0, BLOCK // 1024, pack, 0)


def halves(x, axis):
    high = x.astype(bf16)
    low = (x - high.astype(f32)).astype(bf16)
    return jnp.concatenate([high, low, high], axis=axis)


QUARTER_HIGH = 1.5703125
QUARTER_MID = float(np.float32(np.round((np.pi / 2 - QUARTER_HIGH) * 2**22) / 2**22))
QUARTER_LOW = float(np.float32(np.pi / 2 - QUARTER_HIGH - QUARTER_MID))


def cos_sin(phase):
    turns = jnp.round(phase * (2 / np.pi))
    r = ((phase - turns * QUARTER_HIGH) - turns * QUARTER_MID) - turns * QUARTER_LOW
    quadrant = turns.astype(jnp.int32)
    z = r * r
    s = r + r * z * (-1.6666654611e-1 + z * (8.3321608736e-3 + z * (-1.9515295891e-4)))
    c = 1.0 - 0.5 * z + z * z * (4.166664568298827e-2 + z * (-1.388731625493765e-3 + z * 2.443315711809948e-5))
    odd = (quadrant & 1) == 1
    cos = jnp.where(odd, s, c)
    sin = jnp.where(odd, c, s)
    cos = jnp.where(((quadrant + 1) & 2) == 2, -cos, cos)
    sin = jnp.where((quadrant & 2) == 2, -sin, sin)
    return cos, sin


def dedisperse_kernel(
    sub_ref, dm_ref, x_ref, fl_ref, br_ref, fr_ref, ll_ref, tw_ref, out_ref, time_ref, base_ref, last_ref
):
    for src in range(STA):
        scale = scale_of(widen(x_ref[src, :, BLOCK:])) * (1.0 / LEVELS)

        def decode(i, carry):
            at = pl.multiple_of(i * 512, 512)
            x = widen(x_ref[src, :, pl.ds(at, 512)])
            for u in range(4):
                time_ref[src * TILES + i * 4 + u] = x[:, u * LANES : (u + 1) * LANES] * scale
            return carry

        lax.fori_loop(0, TILES // 4, decode, 0, unroll=2)

    centre = BASE_FREQ + CHANNEL_WIDTH * (sub_ref[0].astype(f32) + 0.5)
    row = lax.broadcasted_iota(jnp.int32, (ROOT, ROOT), 0)
    col = lax.broadcasted_iota(jnp.int32, (ROOT, ROOT), 1)
    k1 = 2 * (row & (HALF - 1)) + lax.shift_right_logical(row, 7)
    k2 = 2 * (col & (HALF - 1)) + lax.shift_right_logical(col, 7)
    position = k1 + ROOT * k2
    signed = jnp.where(position < TOTAL // 2, position, position - TOTAL)
    offset = CHANNEL_WIDTH * signed.astype(f32) / TOTAL
    base_ref[...] = (TWO_PI * DISPERSION) * offset * offset / (centre * centre * (centre + offset))

    flat = time_ref.reshape(TOTAL // LANES * 8, LANES)
    for b in range(BEAMS):
        x = []
        for p in range(2):
            x.append(
                jnp.concatenate([flat[pl.ds(h * 8 + p * 4 + b, ROOT, stride=16), :] for h in range(2)], axis=1)
            )
        outs = []
        for parity in range(2):
            u = [v[:HALF] + v[HALF:] if parity == 0 else v[:HALF] - v[HALF:] for v in x]
            u = jnp.concatenate(u, axis=0)
            outs.append(jnp.dot(fl_ref[parity], halves(u, 0), preferred_element_type=f32))
        re = jnp.concatenate([o[:HALF] for o in outs], axis=0)
        im = jnp.concatenate([o[HALF:] for o in outs], axis=0)
        tw_re, tw_im = tw_ref[0], tw_ref[1]
        re, im = re * tw_re + im * tw_im, im * tw_re - re * tw_im
        outs = []
        for parity in range(2):
            u = [v[:, :HALF] + v[:, HALF:] if parity == 0 else v[:, :HALF] - v[:, HALF:] for v in (re, im)]
            u = jnp.concatenate(u, axis=1)
            outs.append(jnp.dot(halves(u, 1), br_ref[parity], preferred_element_type=f32))
        measure = DM_STEP * dm_ref[b, 0].astype(f32)
        sums = []
        for parity in range(2):
            at = slice(parity * HALF, (parity + 1) * HALF)
            c, s = cos_sin(measure * base_ref[:, at])
            y_re, y_im = outs[parity][:, :HALF], outs[parity][:, HALF:]
            u = jnp.concatenate([y_re * c - y_im * s, y_re * s + y_im * c], axis=1)
            sums.append(jnp.dot(halves(u, 1), fr_ref[parity], preferred_element_type=f32))
        top, bottom = sums[0] + sums[1], sums[0] - sums[1]
        re = jnp.concatenate([top[:, :HALF], bottom[:, :HALF]], axis=1)
        im = jnp.concatenate([top[:, HALF:], bottom[:, HALF:]], axis=1)
        re, im = re * tw_re - im * tw_im, im * tw_re + re * tw_im
        sums = []
        for parity in range(2):
            at = slice(parity * HALF, (parity + 1) * HALF)
            u = jnp.concatenate([re[at], im[at]], axis=0)
            sums.append(jnp.dot(ll_ref[parity], halves(u, 0), preferred_element_type=f32))
        top = (sums[0] + sums[1]) * (1.0 / TOTAL)
        bottom = (sums[0] - sums[1]) * (1.0 / TOTAL)
        for p in range(2):
            for r in range(2):
                at = slice(p * HALF + r * 64, p * HALF + r * 64 + 64)
                for h in range(2):
                    lanes = slice(h * LANES, (h + 1) * LANES)
                    first = b * 4 + r * 2 + h
                    last_ref[p, pl.ds(first, 64, stride=16), :] = top[at, lanes]
                    last_ref[p, pl.ds(64 * 16 + first, 64, stride=16), :] = bottom[at, lanes]

    def encode(i, carry):
        for u in range(4):
            d = i * 4 + u
            at = pl.ds(pl.multiple_of(d * 16, 16), 16)
            x = [last_ref[0, at, :], last_ref[1, at, :]]
            peak = jnp.maximum(jnp.abs(x[0]), jnp.abs(x[1]))
            peak = jnp.maximum(peak[:8], peak[8:])
            code = code_of(peak)
            inverse = LEVELS / scale_of(code)
            inverse = jnp.concatenate([inverse, inverse], axis=0)
            for p in range(2):
                out_ref[d, p * 16 : p * 16 + 16, :] = quantize(x[p], inverse)
            out_ref[d, 32:40, :] = code.astype(jnp.int32).astype(jnp.int16)
        return carry

    lax.fori_loop(0, DEVICES // 4, encode, 0)


def finish_kernel(x_ref, out_ref, power_ref):
    step = pl.program_id(0)

    @pl.when(step == 0)
    def _():
        power_ref[...] = jnp.zeros_like(power_ref)

    for sta in range(STA):
        scale = scale_of(widen(x_ref[sta, 32:40, :])) * (1.0 / LEVELS)
        scale = jnp.concatenate([scale, scale], axis=0)
        re = widen(x_ref[sta, 0:16, :]) * scale
        im = widen(x_ref[sta, 16:32, :]) * scale
        out_ref[sta * 16 : sta * 16 + 16, :] = re
        out_ref[128 + sta * 16 : 128 + sta * 16 + 16, :] = im
        power_ref[sta * 16 : sta * 16 + 16, :] += re * re + im * im

    @pl.when(step == pl.num_programs(0) - 1)
    def _():
        power_ref[...] = power_ref[...] * (1.0 / 16.0)


VMEM = pl.BlockSpec(memory_space=pltpu.VMEM)
SMEM = pl.BlockSpec(memory_space=pltpu.SMEM)
PARAMS = pltpu.CompilerParams(vmem_limit_bytes=48 * 1024 * 1024)


def shift(voltages, delays):
    return pl.pallas_call(
        shift_kernel,
        out_shape=jax.ShapeDtypeStruct((STA, 2, STA, BLOCK), bf16),
        in_specs=[SMEM, VMEM],
        out_specs=VMEM,
        scratch_shapes=[pltpu.VMEM((TOTAL // LANES + 128, STA, LANES), f32)],
        compiler_params=PARAMS,
        name="shift",
    )(delays, voltages)


def beamform(volts, weights):
    return pl.pallas_call(
        beam_kernel,
        out_shape=jax.ShapeDtypeStruct((STA, 8, BLOCK + LANES), jnp.int16),
        in_specs=[VMEM, VMEM],
        out_specs=VMEM,
        scratch_shapes=[pltpu.VMEM((64, BLOCK), f32)],
        compiler_params=PARAMS,
        name="beamform",
    )(volts, weights)


def dedisperse(subband, dm_index, coded):
    fl, br, fr, ll, tw = tables()
    return pl.pallas_call(
        dedisperse_kernel,
        out_shape=jax.ShapeDtypeStruct((DEVICES, 40, LANES), jnp.int16),
        in_specs=[SMEM, SMEM] + [VMEM] * 6,
        out_specs=VMEM,
        scratch_shapes=[
            pltpu.VMEM((TOTAL // LANES, 8, LANES), f32),
            pltpu.VMEM((ROOT, ROOT), f32),
            pltpu.VMEM((2, DEVICES * 16, LANES), f32),
        ],
        compiler_params=PARAMS,
        name="dedisperse",
    )(subband, dm_index, coded, fl, br, fr, ll, tw)


def finish(coded):
    return pl.pallas_call(
        finish_kernel,
        grid=(16,),
        out_shape=(jax.ShapeDtypeStruct((4096, LANES), f32), jax.ShapeDtypeStruct((128, LANES), f32)),
        in_specs=[pl.BlockSpec((STA, 40, LANES), lambda s: (s, 0, 0))],
        out_specs=(
            pl.BlockSpec((256, LANES), lambda s: (s, 0)),
            pl.BlockSpec((128, LANES), lambda s: (0, 0)),
        ),
        compiler_params=PARAMS,
        name="finish",
    )(coded)


def shards(voltages, beam_weights, station_delays, dm_index):
    shifted = shift(voltages, station_delays)
    volts = lax.all_to_all(shifted, "sta", 0, 0, tiled=True)
    coded = beamform(volts, beam_weights)
    coded = lax.all_to_all(coded, "sta", 0, 0, tiled=True)
    subband = lax.axis_index("sub").astype(jnp.int32).reshape(1)
    coded = dedisperse(subband, dm_index, coded)
    coded = lax.all_to_all(coded, ("sub", "sta"), 0, 0, tiled=True)
    moved, intensity = finish(coded)
    return moved.reshape(16, 2, 32, 1, 512), intensity.reshape(32, 1, 512)


def solution(mesh):
    return jax.shard_map(
        shards,
        mesh=mesh,
        in_specs=(
            P("sub", None, "sta", None),
            P("sub", None, None, None),
            P("sta"),
            P("sta", None),
        ),
        out_specs=(P(None, None, None, None, ("sub", "sta")), P(None, None, ("sub", "sta"))),
        check_vma=False,
    )
```

```python
import functools

import jax
import jax.numpy as jnp
import numpy as np
from jax import lax
from jax.experimental import pallas as pl
from jax.experimental.pallas import tpu as pltpu
from jax.sharding import PartitionSpec as P

TWO_PI = 6.283185307179586
DISPERSION = 4148808000.0
DM_STEP = 10.0
BASE_FREQ = 120.0
CHANNEL_WIDTH = 0.1953125

TOTAL = 65536
ROOT = 256
HALF = 128
LANES = 128
STA = 8
BLOCK = TOTAL // STA
TILES = BLOCK // LANES
BEAMS = 4
DEVICES = 128
CODE_STEP = 64.0
LEVELS = 32767.0
FLOOR = 1e-33

f32 = jnp.float32
bf16 = jnp.bfloat16


def split_np(table):
    high = table.astype(bf16)
    low = (table - high.astype(np.float64)).astype(bf16)
    return high, low


@functools.lru_cache(maxsize=None)
def tables():
    m = np.arange(HALF)
    fwd = []
    for parity in range(2):
        angle = 2 * np.pi * (((2 * m[:, None] + parity) * m[None, :]) % ROOT) / ROOT
        c, s = np.cos(angle), np.sin(angle)
        fwd.append(np.block([[c, s], [-s, c]]))
    fwd = np.stack(fwd)
    bwd = fwd.transpose(0, 2, 1)
    order = (2 * np.arange(64)[None, :] + np.arange(2)[:, None]).reshape(-1)
    order = np.concatenate([order, HALF + order])
    last = bwd[:, order, :]

    def pair(t):
        return np.stack(split_np(t), axis=1)

    rows = np.concatenate([2 * m, 2 * m + 1])
    angle = 2 * np.pi * (rows[:, None] * np.arange(ROOT)[None, :]) / TOTAL
    twiddle = np.stack([np.cos(angle), np.sin(angle)]).astype(np.float32)
    return pair(fwd), pair(bwd), pair(last), twiddle


def code_of(peak):
    return jnp.ceil(jnp.log(jnp.maximum(peak, FLOOR)) * (CODE_STEP / 0.6931471805599453)) + 1.0


def scale_of(code):
    return jnp.exp2(code * (1.0 / CODE_STEP))


def quantize(x, inverse):
    return jnp.round(x * inverse).astype(jnp.int32).astype(jnp.int16)


def widen(q):
    return q.astype(jnp.int32).astype(f32)


FRONT = 136


def shift_kernel(delay_ref, v_ref, out_ref, plain_ref, turned_ref):
    count = TOTAL // LANES
    lane = lax.broadcasted_iota(jnp.int32, (STA, LANES), 1)
    row = lax.broadcasted_iota(jnp.int32, (STA, LANES), 0)
    fine = jnp.zeros((STA, LANES), jnp.int32)
    for q in range(STA):
        fine = jnp.where(row == q, delay_ref[q] & (LANES - 1), fine)
    keep = lane >= fine
    source = lax.broadcasted_iota(jnp.int32, (LANES, LANES), 0)
    target = lax.broadcasted_iota(jnp.int32, (LANES, LANES), 1)
    turn = (target - source) & (LANES - 1)
    unroll = 8
    rows = count + 8
    for p in range(2):
        plain = plain_ref.at[p]
        turned = turned_ref.at[p]

        def fill(i, carry):
            at = pl.multiple_of(i * (unroll * LANES), unroll * LANES)
            x = v_ref[0, p, :, pl.ds(at, unroll * LANES)].astype(f32)
            for u in range(unroll):
                to = pl.multiple_of((FRONT + i * unroll + u) * STA, STA)
                plain[pl.ds(to, STA), :] = x[:, u * LANES : (u + 1) * LANES]
            return carry

        lax.fori_loop(0, count // unroll, fill, 0)
        plain[: FRONT * STA, :] = plain[count * STA : (count + FRONT) * STA, :]
        for q in range(STA):
            fine_q = delay_ref[q] & (LANES - 1)
            coarse_q = lax.shift_right_logical(delay_ref[q], 7)
            matrix = (turn == fine_q).astype(f32).astype(bf16)
            x = plain[pl.ds((FRONT - 8 - coarse_q) * STA + q, rows, stride=STA), :].astype(bf16)
            turned[pl.ds(q, rows, stride=STA), :] = jnp.dot(x, matrix, preferred_element_type=f32)

        def merge(i, before):
            parts = []
            for u in range(unroll):
                now = turned[pl.ds(pl.multiple_of((8 + i * unroll + u) * STA, STA), STA), :]
                parts.append(jnp.where(keep, now, before))
                before = now
            wide = jnp.concatenate(parts, axis=1).astype(bf16)
            d = i // (TILES // unroll)
            at = (i % (TILES // unroll)) * (unroll * LANES)
            out_ref[d, p, :, pl.ds(pl.multiple_of(at, unroll * LANES), unroll * LANES)] = wide
            return before

        lax.fori_loop(0, count // unroll, merge, turned[7 * STA : 8 * STA, :])


def beam_kernel(v_ref, w_ref, out_ref, sums_ref):
    w = w_ref[0].astype(f32)
    rows = []
    for d in range(STA):
        w_re = w[0, d * BEAMS : (d + 1) * BEAMS]
        w_im = w[1, d * BEAMS : (d + 1) * BEAMS]
        rows.append(jnp.concatenate([w_re, -w_im], axis=1))
        rows.append(jnp.concatenate([w_im, w_re], axis=1))
    left = jnp.concatenate(rows, axis=0).astype(bf16)
    chunk = 1024

    def mix(i, peak):
        at = pl.ds(pl.multiple_of(i * chunk, chunk), chunk)
        volts = jnp.concatenate(
            [v_ref[g, 0, :, at] for g in range(STA)] + [v_ref[g, 1, :, at] for g in range(STA)], axis=0
        )
        sums = jnp.dot(left, volts, preferred_element_type=f32)
        sums_ref[:, at] = sums
        for u in range(chunk // LANES):
            peak = jnp.maximum(peak, jnp.abs(sums[:, u * LANES : (u + 1) * LANES]))
        return peak

    peak = lax.fori_loop(0, BLOCK // chunk, mix, jnp.zeros((64, LANES), f32))
    code = code_of(peak)
    inverse = LEVELS / scale_of(code)
    for d in range(STA):
        at8 = slice(d * 8, d * 8 + 8)
        factor = inverse[at8]
        out_ref[d, :, BLOCK:] = code[at8].astype(jnp.int32).astype(jnp.int16)

        def pack(i, carry):
            at = pl.multiple_of(i * 1024, 1024)
            x = sums_ref[at8, pl.ds(at, 1024)]
            x = x * jnp.concatenate([factor] * 8, axis=1)
            out_ref[d, :, pl.ds(at, 1024)] = jnp.round(x).astype(jnp.int32).astype(jnp.int16)
            return carry

        lax.fori_loop(0, BLOCK // 1024, pack, 0)


def halves(x, axis):
    high = x.astype(bf16)
    low = (x - high.astype(f32)).astype(bf16)
    return jnp.concatenate([high, low, high], axis=axis)


def dot_left(table_ref, parity, u):
    high, low = table_ref[parity, 0], table_ref[parity, 1]
    return jnp.dot(jnp.concatenate([high, high, low], axis=1), halves(u, 0), preferred_element_type=f32)


def dot_right(u, table_ref, parity):
    high, low = table_ref[parity, 0], table_ref[parity, 1]
    return jnp.dot(halves(u, 1), jnp.concatenate([high, high, low], axis=0), preferred_element_type=f32)


QUARTER_HIGH = 1.5703125
QUARTER_MID = float(np.float32(np.round((np.pi / 2 - QUARTER_HIGH) * 2**22) / 2**22))
QUARTER_LOW = float(np.float32(np.pi / 2 - QUARTER_HIGH - QUARTER_MID))


def cos_sin(phase):
    turns = jnp.round(phase * (2 / np.pi))
    r = ((phase - turns * QUARTER_HIGH) - turns * QUARTER_MID) - turns * QUARTER_LOW
    quadrant = turns.astype(jnp.int32)
    z = r * r
    s = r + r * z * (-1.6666654611e-1 + z * (8.3321608736e-3 + z * (-1.9515295891e-4)))
    c = 1.0 - 0.5 * z + z * z * (4.166664568298827e-2 + z * (-1.388731625493765e-3 + z * 2.443315711809948e-5))
    odd = (quadrant & 1) == 1
    cos = jnp.where(odd, s, c)
    sin = jnp.where(odd, c, s)
    cos = jnp.where(((quadrant + 1) & 2) == 2, -cos, cos)
    sin = jnp.where((quadrant & 2) == 2, -sin, sin)
    return cos, sin


def dedisperse_kernel(
    sub_ref, dm_ref, x_ref, fwd_ref, bwd_ref, end_ref, tw_ref, out_ref, time_ref, base_ref, last_ref
):
    for src in range(STA):
        scale = scale_of(widen(x_ref[src, :, BLOCK:])) * (1.0 / LEVELS)

        def decode(i, carry):
            at = pl.multiple_of(i * 512, 512)
            x = widen(x_ref[src, :, pl.ds(at, 512)])
            for u in range(4):
                time_ref[src * TILES + i * 4 + u] = x[:, u * LANES : (u + 1) * LANES] * scale
            return carry

        lax.fori_loop(0, TILES // 4, decode, 0, unroll=2)

    centre = BASE_FREQ + CHANNEL_WIDTH * (sub_ref[0].astype(f32) + 0.5)
    row = lax.broadcasted_iota(jnp.int32, (ROOT, ROOT), 0)
    col = lax.broadcasted_iota(jnp.int32, (ROOT, ROOT), 1)
    k1 = 2 * (row & (HALF - 1)) + lax.shift_right_logical(row, 7)
    k2 = 2 * (col & (HALF - 1)) + lax.shift_right_logical(col, 7)
    position = k1 + ROOT * k2
    signed = jnp.where(position < TOTAL // 2, position, position - TOTAL)
    offset = CHANNEL_WIDTH * signed.astype(f32) / TOTAL
    base_ref[...] = (TWO_PI * DISPERSION) * offset * offset / (centre * centre * (centre + offset))

    flat = time_ref.reshape(TOTAL // LANES * 8, LANES)
    for b in range(BEAMS):
        x = []
        for p in range(2):
            x.append(
                jnp.concatenate([flat[pl.ds(h * 8 + p * 4 + b, ROOT, stride=16), :] for h in range(2)], axis=1)
            )
        outs = []
        for parity in range(2):
            u = [v[:HALF] + v[HALF:] if parity == 0 else v[:HALF] - v[HALF:] for v in x]
            u = jnp.concatenate(u, axis=0)
            outs.append(dot_left(fwd_ref, parity, u))
        re = jnp.concatenate([o[:HALF] for o in outs], axis=0)
        im = jnp.concatenate([o[HALF:] for o in outs], axis=0)
        tw_re, tw_im = tw_ref[0], tw_ref[1]
        re, im = re * tw_re + im * tw_im, im * tw_re - re * tw_im
        outs = []
        for parity in range(2):
            u = [v[:, :HALF] + v[:, HALF:] if parity == 0 else v[:, :HALF] - v[:, HALF:] for v in (re, im)]
            u = jnp.concatenate(u, axis=1)
            outs.append(dot_right(u, bwd_ref, parity))
        measure = DM_STEP * dm_ref[b, 0].astype(f32)
        sums = []
        for parity in range(2):
            at = slice(parity * HALF, (parity + 1) * HALF)
            c, s = cos_sin(measure * base_ref[:, at])
            y_re, y_im = outs[parity][:, :HALF], outs[parity][:, HALF:]
            u = jnp.concatenate([y_re * c - y_im * s, y_re * s + y_im * c], axis=1)
            sums.append(dot_right(u, fwd_ref, parity))
        top, bottom = sums[0] + sums[1], sums[0] - sums[1]
        re = jnp.concatenate([top[:, :HALF], bottom[:, :HALF]], axis=1)
        im = jnp.concatenate([top[:, HALF:], bottom[:, HALF:]], axis=1)
        re, im = re * tw_re - im * tw_im, im * tw_re + re * tw_im
        sums = []
        for parity in range(2):
            at = slice(parity * HALF, (parity + 1) * HALF)
            u = jnp.concatenate([re[at], im[at]], axis=0)
            sums.append(dot_left(end_ref, parity, u))
        top = (sums[0] + sums[1]) * (1.0 / TOTAL)
        bottom = (sums[0] - sums[1]) * (1.0 / TOTAL)
        for p in range(2):
            for r in range(2):
                at = slice(p * HALF + r * 64, p * HALF + r * 64 + 64)
                for h in range(2):
                    lanes = slice(h * LANES, (h + 1) * LANES)
                    first = b * 4 + r * 2 + h
                    last_ref[p, pl.ds(first, 64, stride=16), :] = top[at, lanes]
                    last_ref[p, pl.ds(64 * 16 + first, 64, stride=16), :] = bottom[at, lanes]

    def encode(i, carry):
        for u in range(4):
            d = i * 4 + u
            at = pl.ds(pl.multiple_of(d * 16, 16), 16)
            x = [last_ref[0, at, :], last_ref[1, at, :]]
            peak = jnp.maximum(jnp.abs(x[0]), jnp.abs(x[1]))
            peak = jnp.maximum(peak[:8], peak[8:])
            code = code_of(peak)
            inverse = LEVELS / scale_of(code)
            inverse = jnp.concatenate([inverse, inverse], axis=0)
            for p in range(2):
                out_ref[d, p * 16 : p * 16 + 16, :] = quantize(x[p], inverse)
            out_ref[d, 32:40, :] = code.astype(jnp.int32).astype(jnp.int16)
        return carry

    lax.fori_loop(0, DEVICES // 4, encode, 0)


SUBS = 4


def finish_kernel(x_ref, out_ref, power_ref):
    step = pl.program_id(0)

    @pl.when(step == 0)
    def _():
        power_ref[...] = jnp.zeros_like(power_ref)

    for sta in range(STA):
        power = power_ref[sta * 16 : sta * 16 + 16, :]
        for sub in range(SUBS):
            src = sub * STA + sta
            to = sub * 256 + sta * 16
            scale = scale_of(widen(x_ref[src, 32:40, :])) * (1.0 / LEVELS)
            scale = jnp.concatenate([scale, scale], axis=0)
            re = widen(x_ref[src, 0:16, :]) * scale
            im = widen(x_ref[src, 16:32, :]) * scale
            out_ref[to : to + 16, :] = re
            out_ref[to + 128 : to + 144, :] = im
            power = power + (re * re + im * im)
        power_ref[sta * 16 : sta * 16 + 16, :] = power

    @pl.when(step == pl.num_programs(0) - 1)
    def _():
        power_ref[...] = power_ref[...] * (1.0 / 16.0)


VMEM = pl.BlockSpec(memory_space=pltpu.VMEM)
SMEM = pl.BlockSpec(memory_space=pltpu.SMEM)
PARAMS = pltpu.CompilerParams(vmem_limit_bytes=48 * 1024 * 1024)


def shift(voltages, delays):
    return pl.pallas_call(
        shift_kernel,
        out_shape=jax.ShapeDtypeStruct((STA, 2, STA, BLOCK), bf16),
        in_specs=[SMEM, VMEM],
        out_specs=VMEM,
        scratch_shapes=[
            pltpu.VMEM((2, (TOTAL // LANES + FRONT) * STA, LANES), f32),
            pltpu.VMEM((2, (TOTAL // LANES + 8) * STA, LANES), f32),
        ],
        compiler_params=PARAMS,
        name="shift",
    )(delays, voltages)


def beamform(volts, weights):
    return pl.pallas_call(
        beam_kernel,
        out_shape=jax.ShapeDtypeStruct((STA, 8, BLOCK + LANES), jnp.int16),
        in_specs=[VMEM, VMEM],
        out_specs=VMEM,
        scratch_shapes=[pltpu.VMEM((64, BLOCK), f32)],
        compiler_params=PARAMS,
        name="beamform",
    )(volts, weights)


def dedisperse(subband, dm_index, coded):
    fwd, bwd, end, tw = tables()
    return pl.pallas_call(
        dedisperse_kernel,
        out_shape=jax.ShapeDtypeStruct((DEVICES, 40, LANES), jnp.int16),
        in_specs=[SMEM, SMEM] + [VMEM] * 5,
        out_specs=VMEM,
        scratch_shapes=[
            pltpu.VMEM((TOTAL // LANES, 8, LANES), f32),
            pltpu.VMEM((ROOT, ROOT), f32),
            pltpu.VMEM((2, DEVICES * 16, LANES), f32),
        ],
        compiler_params=PARAMS,
        name="dedisperse",
    )(subband, dm_index, coded, fwd, bwd, end, tw)


def finish(coded):
    return pl.pallas_call(
        finish_kernel,
        grid=(16 // SUBS,),
        out_shape=(jax.ShapeDtypeStruct((4096, LANES), f32), jax.ShapeDtypeStruct((128, LANES), f32)),
        in_specs=[pl.BlockSpec((SUBS * STA, 40, LANES), lambda s: (s, 0, 0))],
        out_specs=(
            pl.BlockSpec((SUBS * 256, LANES), lambda s: (s, 0)),
            pl.BlockSpec((128, LANES), lambda s: (0, 0)),
        ),
        compiler_params=PARAMS,
        name="finish",
    )(coded)


def shards(voltages, beam_weights, station_delays, dm_index):
    shifted = shift(voltages, station_delays)
    volts = lax.all_to_all(shifted, "sta", 0, 0, tiled=True)
    coded = beamform(volts, beam_weights)
    coded = lax.all_to_all(coded, "sta", 0, 0, tiled=True)
    subband = lax.axis_index("sub").astype(jnp.int32).reshape(1)
    coded = dedisperse(subband, dm_index, coded)
    coded = lax.all_to_all(coded, ("sub", "sta"), 0, 0, tiled=True)
    moved, intensity = finish(coded)
    return moved.reshape(16, 2, 32, 1, 512), intensity.reshape(32, 1, 512)


def solution(mesh):
    return jax.shard_map(
        shards,
        mesh=mesh,
        in_specs=(
            P("sub", None, "sta", None),
            P("sub", None, None, None),
            P("sta"),
            P("sta", None),
        ),
        out_specs=(P(None, None, None, None, ("sub", "sta")), P(None, None, ("sub", "sta"))),
        check_vma=False,
    )
```

```python
import functools

import jax
import jax.numpy as jnp
import numpy as np
from jax import lax
from jax.experimental import pallas as pl
from jax.experimental.pallas import tpu as pltpu
from jax.sharding import PartitionSpec as P

TWO_PI = 6.283185307179586
DISPERSION = 4148808000.0
DM_STEP = 10.0
BASE_FREQ = 120.0
CHANNEL_WIDTH = 0.1953125

TOTAL = 65536
ROOT = 256
HALF = 128
LANES = 128
STA = 8
BLOCK = TOTAL // STA
TILES = BLOCK // LANES
BEAMS = 4
DEVICES = 128
ROWS = 17
CODE_STEP = 64.0
LEVELS = 32767.0
FLOOR = 1e-33

f32 = jnp.float32
bf16 = jnp.bfloat16


def split_np(table):
    high = table.astype(bf16)
    low = (table - high.astype(np.float64)).astype(bf16)
    return high, low


@functools.lru_cache(maxsize=None)
def tables():
    m = np.arange(HALF)
    fwd = []
    for parity in range(2):
        angle = 2 * np.pi * (((2 * m[:, None] + parity) * m[None, :]) % ROOT) / ROOT
        c, s = np.cos(angle), np.sin(angle)
        fwd.append(np.block([[c, s], [-s, c]]))
    fwd = np.stack(fwd)
    bwd = fwd.transpose(0, 2, 1)
    order = (2 * np.arange(64)[None, :] + np.arange(2)[:, None]).reshape(-1)
    order = np.concatenate([order, HALF + order])
    last = bwd[:, order, :]

    def pair(t):
        return np.stack(split_np(t), axis=1)

    rows = np.concatenate([2 * m, 2 * m + 1])
    angle = 2 * np.pi * (rows[:, None] * np.arange(ROOT)[None, :]) / TOTAL
    twiddle = np.stack([np.cos(angle), np.sin(angle)]).astype(np.float32)
    return pair(fwd), pair(bwd), pair(last), twiddle


def code_of(peak):
    return jnp.ceil(jnp.log(jnp.maximum(peak, FLOOR)) * (CODE_STEP / 0.6931471805599453)) + 1.0


def scale_of(code):
    return jnp.exp2(code * (1.0 / CODE_STEP))


def quantize(x, inverse):
    return jnp.round(x * inverse).astype(jnp.int32).astype(jnp.int16)


def widen(q):
    return q.astype(jnp.int32).astype(f32)


FRONT = 136


def shift_kernel(delay_hbm, v_hbm, out_ref, v_ref, delay_ref, plain_ref, turned_ref, sems):
    copies = [pltpu.make_async_copy(v_hbm.at[0, p], v_ref.at[p], sems.at[p]) for p in range(2)]
    copies[0].start()
    delays = pltpu.make_async_copy(delay_hbm, delay_ref, sems.at[2])
    delays.start()
    copies[1].start()
    delays.wait()
    count = TOTAL // LANES
    lane = lax.broadcasted_iota(jnp.int32, (STA, LANES), 1)
    row = lax.broadcasted_iota(jnp.int32, (STA, LANES), 0)
    fine = jnp.zeros((STA, LANES), jnp.int32)
    for q in range(STA):
        fine = jnp.where(row == q, delay_ref[q] & (LANES - 1), fine)
    keep = lane >= fine
    source = lax.broadcasted_iota(jnp.int32, (LANES, LANES), 0)
    target = lax.broadcasted_iota(jnp.int32, (LANES, LANES), 1)
    turn = (target - source) & (LANES - 1)
    none = jnp.zeros((LANES, LANES), bf16)
    matrices = []
    for q in range(0, STA, 2):
        pair = [(turn == (delay_ref[q + i] & (LANES - 1))).astype(f32).astype(bf16) for i in range(2)]
        top = jnp.concatenate([pair[0], none], axis=1)
        low = jnp.concatenate([none, pair[1]], axis=1)
        matrices.append(jnp.concatenate([top, low], axis=0))
    unroll = 8
    rows = count + 8
    for p in range(2):
        plain = plain_ref.at[p]
        turned = turned_ref.at[p]
        copies[p].wait()

        def fill(i, carry):
            at = pl.multiple_of(i * (unroll * LANES), unroll * LANES)
            x = v_ref[p, :, pl.ds(at, unroll * LANES)].astype(f32)
            for u in range(unroll):
                to = pl.multiple_of((FRONT + i * unroll + u) * STA, STA)
                plain[pl.ds(to, STA), :] = x[:, u * LANES : (u + 1) * LANES]
            return carry

        lax.fori_loop(0, count // unroll, fill, 0, unroll=2)
        plain[: FRONT * STA, :] = plain[count * STA : (count + FRONT) * STA, :]
        for q in range(0, STA, 2):
            x = []
            for i in range(2):
                coarse = lax.shift_right_logical(delay_ref[q + i], 7)
                first = (FRONT - 8 - coarse) * STA + q + i
                x.append(plain[pl.ds(first, rows, stride=STA), :].astype(bf16))
            y = jnp.dot(jnp.concatenate(x, axis=1), matrices[q // 2], preferred_element_type=f32)
            for i in range(2):
                turned[pl.ds(q + i, rows, stride=STA), :] = y[:, i * LANES : (i + 1) * LANES]

        def merge(i, before):
            parts = []
            for u in range(unroll):
                now = turned[pl.ds(pl.multiple_of((8 + i * unroll + u) * STA, STA), STA), :]
                parts.append(jnp.where(keep, now, before))
                before = now
            wide = jnp.concatenate(parts, axis=1).astype(bf16)
            d = i // (TILES // unroll)
            at = (i % (TILES // unroll)) * (unroll * LANES)
            out_ref[d, p, :, pl.ds(pl.multiple_of(at, unroll * LANES), unroll * LANES)] = wide
            return before

        lax.fori_loop(0, count // unroll, merge, turned[7 * STA : 8 * STA, :], unroll=2)


def beam_kernel(v_ref, w_ref, out_ref, sums_ref):
    w = w_ref[0].astype(f32)
    rows = []
    for d in range(STA):
        w_re = w[0, d * BEAMS : (d + 1) * BEAMS]
        w_im = w[1, d * BEAMS : (d + 1) * BEAMS]
        rows.append(jnp.concatenate([w_re, -w_im], axis=1))
        rows.append(jnp.concatenate([w_im, w_re], axis=1))
    left = jnp.concatenate(rows, axis=0).astype(bf16)
    chunk = 1024

    def mix(i, peak):
        at = pl.ds(pl.multiple_of(i * chunk, chunk), chunk)
        volts = jnp.concatenate(
            [v_ref[g, 0, :, at] for g in range(STA)] + [v_ref[g, 1, :, at] for g in range(STA)], axis=0
        )
        sums = jnp.dot(left, volts, preferred_element_type=f32)
        sums_ref[:, at] = sums
        for u in range(chunk // LANES):
            peak = jnp.maximum(peak, jnp.abs(sums[:, u * LANES : (u + 1) * LANES]))
        return peak

    peak = lax.fori_loop(0, BLOCK // chunk, mix, jnp.zeros((64, LANES), f32))
    code = code_of(peak)
    inverse = LEVELS / scale_of(code)
    for d in range(STA):
        at8 = slice(d * 8, d * 8 + 8)
        factor = inverse[at8]
        out_ref[d, :, BLOCK:] = code[at8].astype(jnp.int32).astype(jnp.int16)

        def pack(i, carry):
            at = pl.multiple_of(i * 1024, 1024)
            x = sums_ref[at8, pl.ds(at, 1024)]
            x = x * jnp.concatenate([factor] * 8, axis=1)
            out_ref[d, :, pl.ds(at, 1024)] = jnp.round(x).astype(jnp.int32).astype(jnp.int16)
            return carry

        lax.fori_loop(0, BLOCK // 1024, pack, 0)


def halves(x, axis):
    high = x.astype(bf16)
    low = (x - high.astype(f32)).astype(bf16)
    return jnp.concatenate([high, low, high], axis=axis)


def dot_left(table_ref, parity, u):
    high, low = table_ref[parity, 0], table_ref[parity, 1]
    return jnp.dot(jnp.concatenate([high, high, low], axis=1), halves(u, 0), preferred_element_type=f32)


def dot_right(u, table_ref, parity):
    high, low = table_ref[parity, 0], table_ref[parity, 1]
    return jnp.dot(halves(u, 1), jnp.concatenate([high, high, low], axis=0), preferred_element_type=f32)


QUARTER_HIGH = 1.5703125
QUARTER_MID = float(np.float32(np.round((np.pi / 2 - QUARTER_HIGH) * 2**22) / 2**22))
QUARTER_LOW = float(np.float32(np.pi / 2 - QUARTER_HIGH - QUARTER_MID))


def cos_sin(phase):
    turns = jnp.round(phase * (2 / np.pi))
    r = ((phase - turns * QUARTER_HIGH) - turns * QUARTER_MID) - turns * QUARTER_LOW
    quadrant = turns.astype(jnp.int32)
    z = r * r
    s = r + r * z * (-1.6666654611e-1 + z * (8.3321608736e-3 + z * (-1.9515295891e-4)))
    c = 1.0 - 0.5 * z + z * z * (4.166664568298827e-2 + z * (-1.388731625493765e-3 + z * 2.443315711809948e-5))
    odd = (quadrant & 1) == 1
    cos = jnp.where(odd, s, c)
    sin = jnp.where(odd, c, s)
    cos = jnp.where(((quadrant + 1) & 2) == 2, -cos, cos)
    sin = jnp.where((quadrant & 2) == 2, -sin, sin)
    return cos, sin


def dedisperse_kernel(
    dm_ref, x_ref, fwd_ref, bwd_ref, end_ref, tw_ref, out_ref, time_ref, base_ref, last_ref
):
    for src in range(STA):
        scale = scale_of(widen(x_ref[src, :, BLOCK:])) * (1.0 / LEVELS)

        def decode(i, carry):
            at = pl.multiple_of(i * 512, 512)
            x = widen(x_ref[src, :, pl.ds(at, 512)])
            for u in range(4):
                time_ref[src * TILES + i * 4 + u] = x[:, u * LANES : (u + 1) * LANES] * scale
            return carry

        lax.fori_loop(0, TILES // 4, decode, 0, unroll=2)

    centre = BASE_FREQ + CHANNEL_WIDTH * (lax.axis_index("sub").astype(f32) + 0.5)
    row = lax.broadcasted_iota(jnp.int32, (ROOT, ROOT), 0)
    col = lax.broadcasted_iota(jnp.int32, (ROOT, ROOT), 1)
    k1 = 2 * (row & (HALF - 1)) + lax.shift_right_logical(row, 7)
    k2 = 2 * (col & (HALF - 1)) + lax.shift_right_logical(col, 7)
    position = k1 + ROOT * k2
    signed = jnp.where(position < TOTAL // 2, position, position - TOTAL)
    offset = CHANNEL_WIDTH * signed.astype(f32) / TOTAL
    base_ref[...] = (TWO_PI * DISPERSION) * offset * offset / (centre * centre * (centre + offset))

    flat = time_ref.reshape(TOTAL // LANES * 8, LANES)
    for b in range(BEAMS):
        x = []
        for p in range(2):
            x.append(
                jnp.concatenate([flat[pl.ds(h * 8 + p * 4 + b, ROOT, stride=16), :] for h in range(2)], axis=1)
            )
        outs = []
        for parity in range(2):
            u = [v[:HALF] + v[HALF:] if parity == 0 else v[:HALF] - v[HALF:] for v in x]
            u = jnp.concatenate(u, axis=0)
            outs.append(dot_left(fwd_ref, parity, u))
        re = jnp.concatenate([o[:HALF] for o in outs], axis=0)
        im = jnp.concatenate([o[HALF:] for o in outs], axis=0)
        tw_re, tw_im = tw_ref[0], tw_ref[1]
        re, im = re * tw_re + im * tw_im, im * tw_re - re * tw_im
        outs = []
        for parity in range(2):
            u = [v[:, :HALF] + v[:, HALF:] if parity == 0 else v[:, :HALF] - v[:, HALF:] for v in (re, im)]
            u = jnp.concatenate(u, axis=1)
            outs.append(dot_right(u, bwd_ref, parity))
        measure = DM_STEP * dm_ref[b].astype(f32)
        sums = []
        for parity in range(2):
            at = slice(parity * HALF, (parity + 1) * HALF)
            c, s = cos_sin(measure * base_ref[:, at])
            y_re, y_im = outs[parity][:, :HALF], outs[parity][:, HALF:]
            u = jnp.concatenate([y_re * c - y_im * s, y_re * s + y_im * c], axis=1)
            sums.append(dot_right(u, fwd_ref, parity))
        top, bottom = sums[0] + sums[1], sums[0] - sums[1]
        re = jnp.concatenate([top[:, :HALF], bottom[:, :HALF]], axis=1)
        im = jnp.concatenate([top[:, HALF:], bottom[:, HALF:]], axis=1)
        re, im = re * tw_re - im * tw_im, im * tw_re + re * tw_im
        sums = []
        for parity in range(2):
            at = slice(parity * HALF, (parity + 1) * HALF)
            u = jnp.concatenate([re[at], im[at]], axis=0)
            sums.append(dot_left(end_ref, parity, u))
        top = (sums[0] + sums[1]) * (1.0 / TOTAL)
        bottom = (sums[0] - sums[1]) * (1.0 / TOTAL)
        for p in range(2):
            for r in range(2):
                at = slice(p * HALF + r * 64, p * HALF + r * 64 + 64)
                for h in range(2):
                    lanes = slice(h * LANES, (h + 1) * LANES)
                    first = b * 4 + r * 2 + h
                    last_ref[p, first, :64] = top[at, lanes]
                    last_ref[p, first, 64:] = bottom[at, lanes]

    def encode(i, carry):
        at = pl.ds(pl.multiple_of(i * 8, 8), 8)
        x = [[last_ref[p, k, at, :] for k in range(16)] for p in range(2)]
        peak = jnp.abs(x[0][0])
        for k in range(1, 32):
            peak = jnp.maximum(peak, jnp.abs(x[k // 16][k % 16]))
        code = code_of(peak)
        inverse = LEVELS / scale_of(code)
        first = i * (8 * ROWS)
        for k in range(16):
            low = jnp.round(x[0][k] * inverse).astype(jnp.int32) & 0xFFFF
            high = jnp.round(x[1][k] * inverse).astype(jnp.int32) << 16
            out_ref[pl.ds(first + k, 8, stride=ROWS), :] = low | high
        out_ref[pl.ds(first + 16, 8, stride=ROWS), :] = code.astype(jnp.int32)
        return carry

    lax.fori_loop(0, DEVICES // 8, encode, 0)


SUBS = 4


def finish_kernel(x_ref, out_ref, power_ref):
    step = pl.program_id(0)

    @pl.when(step == 0)
    def _():
        power_ref[...] = jnp.zeros_like(power_ref)

    scales = []
    for sub in range(SUBS):
        code = x_ref[pl.ds(sub * STA * ROWS + 16, STA, stride=ROWS), :]
        scales.append(scale_of(code.astype(f32)) * (1.0 / LEVELS))
    for sta in range(STA):
        power = power_ref[sta * 16 : sta * 16 + 16, :]
        for sub in range(SUBS):
            src = (sub * STA + sta) * ROWS
            to = sub * 256 + sta * 16
            scale = jnp.broadcast_to(scales[sub][sta : sta + 1], (16, LANES))
            both = x_ref[src : src + 16, :]
            re = ((both << 16) >> 16).astype(f32) * scale
            im = (both >> 16).astype(f32) * scale
            out_ref[to : to + 16, :] = re
            out_ref[to + 128 : to + 144, :] = im
            power = power + (re * re + im * im)
        power_ref[sta * 16 : sta * 16 + 16, :] = power

    @pl.when(step == pl.num_programs(0) - 1)
    def _():
        power_ref[...] = power_ref[...] * (1.0 / 16.0)


VMEM = pl.BlockSpec(memory_space=pltpu.VMEM)
SMEM = pl.BlockSpec(memory_space=pltpu.SMEM)
HBM = pl.BlockSpec(memory_space=pltpu.HBM)
PARAMS = pltpu.CompilerParams(vmem_limit_bytes=48 * 1024 * 1024)


def shift(voltages, delays):
    return pl.pallas_call(
        shift_kernel,
        out_shape=jax.ShapeDtypeStruct((STA, 2, STA, BLOCK), bf16),
        in_specs=[HBM, HBM],
        out_specs=VMEM,
        scratch_shapes=[
            pltpu.VMEM((2, STA, TOTAL), bf16),
            pltpu.SMEM((STA,), jnp.int32),
            pltpu.VMEM((2, (TOTAL // LANES + FRONT) * STA, LANES), f32),
            pltpu.VMEM((2, (TOTAL // LANES + 8) * STA, LANES), f32),
            pltpu.SemaphoreType.DMA((3,)),
        ],
        compiler_params=PARAMS,
        name="shift",
    )(delays, voltages)


def beamform(volts, weights):
    return pl.pallas_call(
        beam_kernel,
        out_shape=jax.ShapeDtypeStruct((STA, 8, BLOCK + LANES), jnp.int16),
        in_specs=[VMEM, VMEM],
        out_specs=VMEM,
        scratch_shapes=[pltpu.VMEM((64, BLOCK), f32)],
        compiler_params=PARAMS,
        name="beamform",
    )(volts, weights)


def dedisperse(dm_index, coded):
    fwd, bwd, end, tw = tables()
    return pl.pallas_call(
        dedisperse_kernel,
        out_shape=jax.ShapeDtypeStruct((DEVICES * ROWS, LANES), jnp.int32),
        in_specs=[SMEM] + [VMEM] * 5,
        out_specs=VMEM,
        scratch_shapes=[
            pltpu.VMEM((TOTAL // LANES, 8, LANES), f32),
            pltpu.VMEM((ROOT, ROOT), f32),
            pltpu.VMEM((2, 16, DEVICES, LANES), f32),
        ],
        compiler_params=PARAMS,
        name="dedisperse",
    )(dm_index, coded, fwd, bwd, end, tw)


def finish(coded):
    return pl.pallas_call(
        finish_kernel,
        grid=(16 // SUBS,),
        out_shape=(jax.ShapeDtypeStruct((4096, LANES), f32), jax.ShapeDtypeStruct((128, LANES), f32)),
        in_specs=[pl.BlockSpec((SUBS * STA * ROWS, LANES), lambda s: (s, 0))],
        out_specs=(
            pl.BlockSpec((SUBS * 256, LANES), lambda s: (s, 0)),
            pl.BlockSpec((128, LANES), lambda s: (0, 0)),
        ),
        compiler_params=PARAMS,
        name="finish",
    )(coded)


def shards(voltages, beam_weights, station_delays, dm_index):
    shifted = shift(voltages, station_delays)
    volts = lax.all_to_all(shifted, "sta", 0, 0, tiled=True)
    coded = beamform(volts, beam_weights)
    coded = lax.all_to_all(coded, "sta", 0, 0, tiled=True)
    coded = dedisperse(dm_index.reshape(BEAMS), coded).reshape(DEVICES, 1, ROWS * LANES)
    coded = lax.all_to_all(coded, ("sub", "sta"), 0, 0, tiled=True).reshape(DEVICES * ROWS, LANES)
    moved, intensity = finish(coded)
    return moved.reshape(16, 2, 32, 1, 512), intensity.reshape(32, 1, 512)


def solution(mesh):
    return jax.shard_map(
        shards,
        mesh=mesh,
        in_specs=(
            P("sub", None, "sta", None),
            P("sub", None, None, None),
            P("sta"),
            P("sta", None),
        ),
        out_specs=(P(None, None, None, None, ("sub", "sta")), P(None, None, ("sub", "sta"))),
        check_vma=False,
    )
```

```python
import functools

import jax
import jax.numpy as jnp
import numpy as np
from jax import lax
from jax.experimental import pallas as pl
from jax.experimental.pallas import tpu as pltpu
from jax.sharding import PartitionSpec as P

TWO_PI = 6.283185307179586
DISPERSION = 4148808000.0
DM_STEP = 10.0
BASE_FREQ = 120.0
CHANNEL_WIDTH = 0.1953125

TOTAL = 65536
ROOT = 256
HALF = 128
LANES = 128
STA = 8
BLOCK = TOTAL // STA
TILES = BLOCK // LANES
BEAMS = 4
DEVICES = 128
ROWS = 17
CODE_STEP = 64.0
LEVELS = 32767.0
FLOOR = 1e-33

f32 = jnp.float32
bf16 = jnp.bfloat16


def split_np(table):
    high = table.astype(bf16)
    low = (table - high.astype(np.float64)).astype(bf16)
    return high, low


@functools.lru_cache(maxsize=None)
def tables():
    m = np.arange(HALF)
    fwd = []
    for parity in range(2):
        angle = 2 * np.pi * (((2 * m[:, None] + parity) * m[None, :]) % ROOT) / ROOT
        c, s = np.cos(angle), np.sin(angle)
        fwd.append(np.block([[c, s], [-s, c]]))
    fwd = np.stack(fwd)
    bwd = fwd.transpose(0, 2, 1)
    order = (2 * np.arange(64)[None, :] + np.arange(2)[:, None]).reshape(-1)
    order = np.concatenate([order, HALF + order])
    last = bwd[:, order, :] / TOTAL

    def pair(t):
        return np.stack(split_np(t), axis=1)

    rows = np.concatenate([2 * m, 2 * m + 1])
    angle = 2 * np.pi * (rows[:, None] * np.arange(ROOT)[None, :]) / TOTAL
    twiddle = np.stack([np.cos(angle), np.sin(angle)]).astype(np.float32)
    return pair(fwd), pair(bwd), pair(last), twiddle


def code_of(peak):
    return jnp.ceil(jnp.log(jnp.maximum(peak, FLOOR)) * (CODE_STEP / 0.6931471805599453)) + 1.0


def scale_of(code):
    return jnp.exp2(code * (1.0 / CODE_STEP))


def quantize(x, inverse):
    return jnp.round(x * inverse).astype(jnp.int32).astype(jnp.int16)


def widen(q):
    return q.astype(jnp.int32).astype(f32)


FRONT = 136


def shift_kernel(delay_hbm, v_hbm, out_ref, v_ref, delay_ref, plain_ref, turned_ref, sems):
    halves_at = [pl.ds(h * (TOTAL // 2), TOTAL // 2) for h in range(2)]
    delays = pltpu.make_async_copy(delay_hbm, delay_ref, sems.at[4])
    delays.start()
    copies = []
    for p in range(2):
        for h in range(2):
            source, to = v_hbm.at[0, p, :, halves_at[h]], v_ref.at[p, :, halves_at[h]]
            copies.append(pltpu.make_async_copy(source, to, sems.at[p * 2 + h]))
            copies[-1].start()
    delays.wait()
    count = TOTAL // LANES
    lane = lax.broadcasted_iota(jnp.int32, (STA, LANES), 1)
    row = lax.broadcasted_iota(jnp.int32, (STA, LANES), 0)
    fine = jnp.zeros((STA, LANES), jnp.int32)
    for q in range(STA):
        fine = jnp.where(row == q, delay_ref[q] & (LANES - 1), fine)
    keep = lane >= fine
    source = lax.broadcasted_iota(jnp.int32, (LANES, LANES), 0)
    target = lax.broadcasted_iota(jnp.int32, (LANES, LANES), 1)
    turn = (target - source) & (LANES - 1)
    none = jnp.zeros((LANES, LANES), bf16)
    matrices = []
    for q in range(0, STA, 2):
        pair = [(turn == (delay_ref[q + i] & (LANES - 1))).astype(f32).astype(bf16) for i in range(2)]
        top = jnp.concatenate([pair[0], none], axis=1)
        low = jnp.concatenate([none, pair[1]], axis=1)
        matrices.append(jnp.concatenate([top, low], axis=0))
    unroll = 8
    rows = count + 8
    steps = count // unroll
    for p in range(2):
        plain = plain_ref.at[p]

        def fill(i, carry):
            at = pl.multiple_of(i * (unroll * LANES), unroll * LANES)
            x = v_ref[p, :, pl.ds(at, unroll * LANES)].astype(f32)
            for u in range(unroll):
                to = pl.multiple_of((FRONT + i * unroll + u) * STA, STA)
                plain[pl.ds(to, STA), :] = x[:, u * LANES : (u + 1) * LANES]
            return carry

        def wrap(i, carry):
            at = pl.multiple_of((TOTAL - FRONT * LANES) + i * (unroll * LANES), unroll * LANES)
            x = v_ref[p, :, pl.ds(at, unroll * LANES)].astype(f32)
            for u in range(unroll):
                to = pl.multiple_of((i * unroll + u) * STA, STA)
                plain[pl.ds(to, STA), :] = x[:, u * LANES : (u + 1) * LANES]
            return carry

        for h in range(2):
            copies[p * 2 + h].wait()
            lax.fori_loop(h * steps // 2, (h + 1) * steps // 2, fill, 0, unroll=4)
        lax.fori_loop(0, FRONT // unroll, wrap, 0, unroll=2)
    for q in range(0, STA, 2):
        for p in range(2):
            x = []
            for i in range(2):
                coarse = lax.shift_right_logical(delay_ref[q + i], 7)
                first = (FRONT - 8 - coarse) * STA + q + i
                x.append(plain_ref.at[p][pl.ds(first, rows, stride=STA), :].astype(bf16))
            y = jnp.dot(jnp.concatenate(x, axis=1), matrices[q // 2], preferred_element_type=f32)
            for i in range(2):
                turned_ref.at[p][pl.ds(q + i, rows, stride=STA), :] = y[:, i * LANES : (i + 1) * LANES]

    def merge(i, before):
        d = i // (TILES // unroll)
        at = (i % (TILES // unroll)) * (unroll * LANES)
        last = []
        for p in range(2):
            parts = []
            old = before[p]
            for u in range(unroll):
                now = turned_ref[p, pl.ds(pl.multiple_of((8 + i * unroll + u) * STA, STA), STA), :]
                parts.append(jnp.where(keep, now, old))
                old = now
            wide = jnp.concatenate(parts, axis=1).astype(bf16)
            out_ref[d, p, :, pl.ds(pl.multiple_of(at, unroll * LANES), unroll * LANES)] = wide
            last.append(old)
        return tuple(last)

    start = tuple(turned_ref[p, 7 * STA : 8 * STA, :] for p in range(2))
    lax.fori_loop(0, steps, merge, start, unroll=2)


def beam_kernel(v_ref, w_ref, out_ref, sums_ref):
    w = w_ref[0].astype(f32)
    rows = []
    for d in range(STA):
        w_re = w[0, d * BEAMS : (d + 1) * BEAMS]
        w_im = w[1, d * BEAMS : (d + 1) * BEAMS]
        rows.append(jnp.concatenate([w_re, -w_im], axis=1))
        rows.append(jnp.concatenate([w_im, w_re], axis=1))
    left = jnp.concatenate(rows, axis=0).astype(bf16)
    chunk = 1024

    def mix(i, peak):
        at = pl.ds(pl.multiple_of(i * chunk, chunk), chunk)
        volts = jnp.concatenate(
            [v_ref[g, 0, :, at] for g in range(STA)] + [v_ref[g, 1, :, at] for g in range(STA)], axis=0
        )
        sums = jnp.dot(left, volts, preferred_element_type=f32)
        sums_ref[:, at] = sums
        for u in range(chunk // LANES):
            peak = jnp.maximum(peak, jnp.abs(sums[:, u * LANES : (u + 1) * LANES]))
        return peak

    peak = lax.fori_loop(0, BLOCK // chunk, mix, jnp.zeros((64, LANES), f32))
    code = code_of(peak)
    inverse = LEVELS / scale_of(code)
    for d in range(STA):
        at8 = slice(d * 8, d * 8 + 8)
        factor = inverse[at8]
        out_ref[d, :, BLOCK:] = code[at8].astype(jnp.int32).astype(jnp.int16)

        def pack(i, carry):
            at = pl.multiple_of(i * 1024, 1024)
            x = sums_ref[at8, pl.ds(at, 1024)]
            x = x * jnp.concatenate([factor] * 8, axis=1)
            out_ref[d, :, pl.ds(at, 1024)] = jnp.round(x).astype(jnp.int32).astype(jnp.int16)
            return carry

        lax.fori_loop(0, BLOCK // 1024, pack, 0)


def halves(x, axis):
    high = x.astype(bf16)
    low = (x - high.astype(f32)).astype(bf16)
    return jnp.concatenate([high, low, high], axis=axis)


def dot_left(table_ref, parity, u):
    high, low = table_ref[parity, 0], table_ref[parity, 1]
    return jnp.dot(jnp.concatenate([high, high, low], axis=1), halves(u, 0), preferred_element_type=f32)


def dot_right(u, table_ref, parity):
    high, low = table_ref[parity, 0], table_ref[parity, 1]
    return jnp.dot(halves(u, 1), jnp.concatenate([high, high, low], axis=0), preferred_element_type=f32)


QUARTER_HIGH = 1.5703125
QUARTER_LOW = float(np.float32(np.pi / 2 - QUARTER_HIGH))


def cos_sin(phase):
    turns = jnp.round(phase * (2 / np.pi))
    r = (phase - turns * QUARTER_HIGH) - turns * QUARTER_LOW
    quadrant = turns.astype(jnp.int32)
    z = r * r
    s = r + r * z * (-1.6666654611e-1 + z * (8.3321608736e-3 + z * (-1.9515295891e-4)))
    c = 1.0 - 0.5 * z + z * z * (4.166664568298827e-2 + z * (-1.388731625493765e-3 + z * 2.443315711809948e-5))
    odd = (quadrant & 1) == 1
    cos = jnp.where(odd, s, c)
    sin = jnp.where(odd, c, s)
    cos = jnp.where(((quadrant + 1) & 2) == 2, -cos, cos)
    sin = jnp.where((quadrant & 2) == 2, -sin, sin)
    return cos, sin


def dedisperse_kernel(
    dm_ref, x_ref, fwd_ref, bwd_ref, end_ref, tw_ref, out_ref, time_ref, base_ref, last_ref
):
    for src in range(STA):
        scale = scale_of(widen(x_ref[src, :, BLOCK:])) * (1.0 / LEVELS)

        def decode(i, carry):
            at = pl.multiple_of(i * 512, 512)
            x = widen(x_ref[src, :, pl.ds(at, 512)])
            for u in range(4):
                time_ref[src * TILES + i * 4 + u] = x[:, u * LANES : (u + 1) * LANES] * scale
            return carry

        lax.fori_loop(0, TILES // 4, decode, 0, unroll=4)

    centre = BASE_FREQ + CHANNEL_WIDTH * (lax.axis_index("sub").astype(f32) + 0.5)
    row = lax.broadcasted_iota(jnp.int32, (ROOT, ROOT), 0)
    col = lax.broadcasted_iota(jnp.int32, (ROOT, ROOT), 1)
    k1 = 2 * (row & (HALF - 1)) + lax.shift_right_logical(row, 7)
    k2 = 2 * (col & (HALF - 1)) + lax.shift_right_logical(col, 7)
    position = k1 + ROOT * k2
    signed = jnp.where(position < TOTAL // 2, position, position - TOTAL)
    offset = CHANNEL_WIDTH * signed.astype(f32) / TOTAL
    base_ref[...] = (TWO_PI * DISPERSION) * offset * offset / (centre * centre * (centre + offset))

    flat = time_ref.reshape(TOTAL // LANES * 8, LANES)
    def beam(b):
        x = []
        for p in range(2):
            x.append(
                jnp.concatenate([flat[pl.ds(h * 8 + p * 4 + b, ROOT, stride=16), :] for h in range(2)], axis=1)
            )
        yield
        outs = []
        for parity in range(2):
            u = [v[:HALF] + v[HALF:] if parity == 0 else v[:HALF] - v[HALF:] for v in x]
            u = jnp.concatenate(u, axis=0)
            outs.append(dot_left(fwd_ref, parity, u))
        yield
        re = jnp.concatenate([o[:HALF] for o in outs], axis=0)
        im = jnp.concatenate([o[HALF:] for o in outs], axis=0)
        tw_re, tw_im = tw_ref[0], tw_ref[1]
        re, im = re * tw_re + im * tw_im, im * tw_re - re * tw_im
        outs = []
        for parity in range(2):
            u = [v[:, :HALF] + v[:, HALF:] if parity == 0 else v[:, :HALF] - v[:, HALF:] for v in (re, im)]
            u = jnp.concatenate(u, axis=1)
            outs.append(dot_right(u, bwd_ref, parity))
        yield
        measure = DM_STEP * dm_ref[b].astype(f32)
        sums = []
        for parity in range(2):
            at = slice(parity * HALF, (parity + 1) * HALF)
            c, s = cos_sin(measure * base_ref[:, at])
            y_re, y_im = outs[parity][:, :HALF], outs[parity][:, HALF:]
            u = jnp.concatenate([y_re * c - y_im * s, y_re * s + y_im * c], axis=1)
            sums.append(dot_right(u, fwd_ref, parity))
        yield
        top, bottom = sums[0] + sums[1], sums[0] - sums[1]
        re = jnp.concatenate([top[:, :HALF], bottom[:, :HALF]], axis=1)
        im = jnp.concatenate([top[:, HALF:], bottom[:, HALF:]], axis=1)
        re, im = re * tw_re - im * tw_im, im * tw_re + re * tw_im
        sums = []
        for parity in range(2):
            at = slice(parity * HALF, (parity + 1) * HALF)
            u = jnp.concatenate([re[at], im[at]], axis=0)
            sums.append(dot_left(end_ref, parity, u))
        yield
        top, bottom = sums[0] + sums[1], sums[0] - sums[1]
        for p in range(2):
            for r in range(2):
                at = slice(p * HALF + r * 64, p * HALF + r * 64 + 64)
                for h in range(2):
                    lanes = slice(h * LANES, (h + 1) * LANES)
                    first = b * 4 + r * 2 + h
                    last_ref[p, first, :64] = top[at, lanes]
                    last_ref[p, first, 64:] = bottom[at, lanes]

    running = [beam(b) for b in range(BEAMS)]
    for tick in range(1 * (BEAMS - 1) + 6):
        for b in range(BEAMS):
            if tick >= 1 * b:
                next(running[b], None)

    def encode(i, carry):
        at = pl.ds(pl.multiple_of(i * 8, 8), 8)
        x = [[last_ref[p, k, at, :] for k in range(16)] for p in range(2)]
        peak = jnp.abs(x[0][0])
        for k in range(1, 32):
            peak = jnp.maximum(peak, jnp.abs(x[k // 16][k % 16]))
        code = code_of(peak)
        inverse = LEVELS / scale_of(code)
        first = i * (8 * ROWS)
        for k in range(16):
            low = jnp.round(x[0][k] * inverse).astype(jnp.int32) & 0xFFFF
            high = jnp.round(x[1][k] * inverse).astype(jnp.int32) << 16
            out_ref[pl.ds(first + k, 8, stride=ROWS), :] = low | high
        out_ref[pl.ds(first + 16, 8, stride=ROWS), :] = code.astype(jnp.int32)
        return carry

    lax.fori_loop(0, DEVICES // 8, encode, 0, unroll=2)


SUBS = 4


def finish_kernel(x_ref, out_ref, power_ref):
    step = pl.program_id(0)

    @pl.when(step == 0)
    def _():
        power_ref[...] = jnp.zeros_like(power_ref)

    scales = []
    for sub in range(SUBS):
        code = x_ref[pl.ds(sub * STA * ROWS + 16, STA, stride=ROWS), :]
        scales.append(scale_of(code.astype(f32)) * (1.0 / LEVELS))
    for sta in range(STA):
        power = power_ref[sta * 16 : sta * 16 + 16, :]
        for sub in range(SUBS):
            src = (sub * STA + sta) * ROWS
            to = sub * 256 + sta * 16
            scale = jnp.broadcast_to(scales[sub][sta : sta + 1], (16, LANES))
            both = x_ref[src : src + 16, :]
            re = ((both << 16) >> 16).astype(f32) * scale
            im = (both >> 16).astype(f32) * scale
            out_ref[to : to + 16, :] = re
            out_ref[to + 128 : to + 144, :] = im
            power = power + (re * re + im * im)
        power_ref[sta * 16 : sta * 16 + 16, :] = power

    @pl.when(step == pl.num_programs(0) - 1)
    def _():
        power_ref[...] = power_ref[...] * (1.0 / 16.0)


VMEM = pl.BlockSpec(memory_space=pltpu.VMEM)
SMEM = pl.BlockSpec(memory_space=pltpu.SMEM)
HBM = pl.BlockSpec(memory_space=pltpu.HBM)
PARAMS = pltpu.CompilerParams(vmem_limit_bytes=48 * 1024 * 1024)


SHIFT_PARAMS = pltpu.CompilerParams(vmem_limit_bytes=50 * 1024 * 1024 + 512 * 1024)


def shift(voltages, delays):
    return pl.pallas_call(
        shift_kernel,
        out_shape=jax.ShapeDtypeStruct((STA, 2, STA, BLOCK), bf16),
        in_specs=[HBM, HBM],
        out_specs=VMEM,
        scratch_shapes=[
            pltpu.VMEM((2, STA, TOTAL), bf16),
            pltpu.SMEM((STA,), jnp.int32),
            pltpu.VMEM((2, (TOTAL // LANES + FRONT) * STA, LANES), f32),
            pltpu.VMEM((2, (TOTAL // LANES + 8) * STA, LANES), f32),
            pltpu.SemaphoreType.DMA((5,)),
        ],
        compiler_params=SHIFT_PARAMS,
        name="shift",
    )(delays, voltages)


def beamform(volts, weights):
    return pl.pallas_call(
        beam_kernel,
        out_shape=jax.ShapeDtypeStruct((STA, 8, BLOCK + LANES), jnp.int16),
        in_specs=[VMEM, VMEM],
        out_specs=VMEM,
        scratch_shapes=[pltpu.VMEM((64, BLOCK), f32)],
        compiler_params=PARAMS,
        name="beamform",
    )(volts, weights)


def dedisperse(dm_index, coded):
    fwd, bwd, end, tw = tables()
    return pl.pallas_call(
        dedisperse_kernel,
        out_shape=jax.ShapeDtypeStruct((DEVICES * ROWS, LANES), jnp.int32),
        in_specs=[SMEM] + [VMEM] * 5,
        out_specs=VMEM,
        scratch_shapes=[
            pltpu.VMEM((TOTAL // LANES, 8, LANES), f32),
            pltpu.VMEM((ROOT, ROOT), f32),
            pltpu.VMEM((2, 16, DEVICES, LANES), f32),
        ],
        compiler_params=PARAMS,
        name="dedisperse",
    )(dm_index, coded, fwd, bwd, end, tw)


def finish(coded):
    return pl.pallas_call(
        finish_kernel,
        grid=(16 // SUBS,),
        out_shape=(jax.ShapeDtypeStruct((4096, LANES), f32), jax.ShapeDtypeStruct((128, LANES), f32)),
        in_specs=[pl.BlockSpec((SUBS * STA * ROWS, LANES), lambda s: (s, 0))],
        out_specs=(
            pl.BlockSpec((SUBS * 256, LANES), lambda s: (s, 0)),
            pl.BlockSpec((128, LANES), lambda s: (0, 0)),
        ),
        compiler_params=PARAMS,
        name="finish",
    )(coded)


def shards(voltages, beam_weights, station_delays, dm_index):
    shifted = shift(voltages, station_delays)
    volts = lax.all_to_all(shifted, "sta", 0, 0, tiled=True)
    coded = beamform(volts, beam_weights)
    coded = lax.all_to_all(coded, "sta", 0, 0, tiled=True)
    coded = dedisperse(dm_index.reshape(BEAMS), coded).reshape(DEVICES, 1, ROWS * LANES)
    coded = lax.all_to_all(coded, ("sub", "sta"), 0, 0, tiled=True).reshape(DEVICES * ROWS, LANES)
    moved, intensity = finish(coded)
    return moved.reshape(16, 2, 32, 1, 512), intensity.reshape(32, 1, 512)


def solution(mesh):
    return jax.shard_map(
        shards,
        mesh=mesh,
        in_specs=(
            P("sub", None, "sta", None),
            P("sub", None, None, None),
            P("sta"),
            P("sta", None),
        ),
        out_specs=(P(None, None, None, None, ("sub", "sta")), P(None, None, ("sub", "sta"))),
        check_vma=False,
    )
```

```python
import functools

import jax
import jax.numpy as jnp
import numpy as np
from jax import lax
from jax.experimental import pallas as pl
from jax.experimental.pallas import tpu as pltpu
from jax.sharding import PartitionSpec as P

TWO_PI = 6.283185307179586
DISPERSION = 4148808000.0
DM_STEP = 10.0
BASE_FREQ = 120.0
CHANNEL_WIDTH = 0.1953125

TOTAL = 65536
ROOT = 256
HALF = 128
LANES = 128
STA = 8
BLOCK = TOTAL // STA
TILES = BLOCK // LANES
BEAMS = 4
DEVICES = 128
ROWS = 17
CODE_STEP = 64.0
LEVELS = 32767.0
FLOOR = 1e-33

HOPS = [(0, 0), (0, 1), (0, 2), (0, 3), (1, 0), (1, 1), (1, 2), (1, 3)]


f32 = jnp.float32
bf16 = jnp.bfloat16


def neighbour(hop, sign):
    me = lax.axis_index("sta")
    x = (lax.shift_right_logical(me, 2) + hop[0]) & 1
    y = ((me & 3) + sign * hop[1]) & 3
    return x * 4 + y


def split_np(table):
    high = table.astype(bf16)
    low = (table - high.astype(np.float64)).astype(bf16)
    return high, low


@functools.lru_cache(maxsize=None)
def tables():
    m = np.arange(HALF)
    fwd = []
    for parity in range(2):
        angle = 2 * np.pi * (((2 * m[:, None] + parity) * m[None, :]) % ROOT) / ROOT
        c, s = np.cos(angle), np.sin(angle)
        fwd.append(np.block([[c, s], [-s, c]]))
    fwd = np.stack(fwd)
    bwd = fwd.transpose(0, 2, 1)
    order = (2 * np.arange(64)[None, :] + np.arange(2)[:, None]).reshape(-1)
    order = np.concatenate([order, HALF + order])
    last = bwd[:, order, :] / TOTAL

    def pair(t):
        return np.stack(split_np(t), axis=1)

    rows = np.concatenate([2 * m, 2 * m + 1])
    angle = 2 * np.pi * (rows[:, None] * np.arange(ROOT)[None, :]) / TOTAL
    twiddle = np.stack([np.cos(angle), np.sin(angle)]).astype(np.float32)
    return pair(fwd), pair(bwd), pair(last), twiddle


def code_of(peak):
    return jnp.ceil(jnp.log(jnp.maximum(peak, FLOOR)) * (CODE_STEP / 0.6931471805599453)) + 1.0


def scale_of(code):
    return jnp.exp2(code * (1.0 / CODE_STEP))


def quantize(x, inverse):
    return jnp.round(x * inverse).astype(jnp.int32).astype(jnp.int16)


def widen(q):
    return q.astype(jnp.int32).astype(f32)


FRONT = 136


def shift_kernel(delay_hbm, v_hbm, *refs):
    out_refs = refs[:STA]
    v_ref, delay_ref, plain_ref, turned_ref, sems = refs[STA:]
    halves_at = [pl.ds(h * (TOTAL // 2), TOTAL // 2) for h in range(2)]
    delays = pltpu.make_async_copy(delay_hbm, delay_ref, sems.at[4])
    delays.start()
    copies = []
    for p in range(2):
        for h in range(2):
            source, to = v_hbm.at[0, p, :, halves_at[h]], v_ref.at[p, :, halves_at[h]]
            copies.append(pltpu.make_async_copy(source, to, sems.at[p * 2 + h]))
            copies[-1].start()
    delays.wait()
    count = TOTAL // LANES
    lane = lax.broadcasted_iota(jnp.int32, (STA, LANES), 1)
    row = lax.broadcasted_iota(jnp.int32, (STA, LANES), 0)
    fine = jnp.zeros((STA, LANES), jnp.int32)
    for q in range(STA):
        fine = jnp.where(row == q, delay_ref[q] & (LANES - 1), fine)
    keep = lane >= fine
    source = lax.broadcasted_iota(jnp.int32, (LANES, LANES), 0)
    target = lax.broadcasted_iota(jnp.int32, (LANES, LANES), 1)
    turn = (target - source) & (LANES - 1)
    none = jnp.zeros((LANES, LANES), bf16)
    matrices = []
    for q in range(0, STA, 2):
        pair = [(turn == (delay_ref[q + i] & (LANES - 1))).astype(f32).astype(bf16) for i in range(2)]
        top = jnp.concatenate([pair[0], none], axis=1)
        low = jnp.concatenate([none, pair[1]], axis=1)
        matrices.append(jnp.concatenate([top, low], axis=0))
    unroll = 8
    rows = count + 8
    steps = count // unroll
    for p in range(2):
        plain = plain_ref.at[p]

        def fill(i, carry):
            at = pl.multiple_of(i * (unroll * LANES), unroll * LANES)
            x = v_ref[p, :, pl.ds(at, unroll * LANES)].astype(f32)
            for u in range(unroll):
                to = pl.multiple_of((FRONT + i * unroll + u) * STA, STA)
                plain[pl.ds(to, STA), :] = x[:, u * LANES : (u + 1) * LANES]
            return carry

        def wrap(i, carry):
            at = pl.multiple_of((TOTAL - FRONT * LANES) + i * (unroll * LANES), unroll * LANES)
            x = v_ref[p, :, pl.ds(at, unroll * LANES)].astype(f32)
            for u in range(unroll):
                to = pl.multiple_of((i * unroll + u) * STA, STA)
                plain[pl.ds(to, STA), :] = x[:, u * LANES : (u + 1) * LANES]
            return carry

        for h in range(2):
            copies[p * 2 + h].wait()
            lax.fori_loop(h * steps // 2, (h + 1) * steps // 2, fill, 0, unroll=4)
        lax.fori_loop(0, FRONT // unroll, wrap, 0, unroll=2)
    for q in range(0, STA, 2):
        for p in range(2):
            x = []
            for i in range(2):
                coarse = lax.shift_right_logical(delay_ref[q + i], 7)
                first = (FRONT - 8 - coarse) * STA + q + i
                x.append(plain_ref.at[p][pl.ds(first, rows, stride=STA), :].astype(bf16))
            y = jnp.dot(jnp.concatenate(x, axis=1), matrices[q // 2], preferred_element_type=f32)
            for i in range(2):
                turned_ref.at[p][pl.ds(q + i, rows, stride=STA), :] = y[:, i * LANES : (i + 1) * LANES]

    for out_ref, hop in zip(out_refs, HOPS):
        first = neighbour(hop, 1) * TILES

        def merge(i, before):
            at = pl.multiple_of(i * (unroll * LANES), unroll * LANES)
            last = []
            for p in range(2):
                parts = []
                old = before[p]
                for u in range(unroll):
                    tile = 8 + first + i * unroll + u
                    now = turned_ref[p, pl.ds(pl.multiple_of(tile * STA, STA), STA), :]
                    parts.append(jnp.where(keep, now, old))
                    old = now
                out_ref[p, :, pl.ds(at, unroll * LANES)] = jnp.concatenate(parts, axis=1).astype(bf16)
                last.append(old)
            return tuple(last)

        start = tuple(turned_ref[p, pl.ds(pl.multiple_of((7 + first) * STA, STA), STA), :] for p in range(2))
        lax.fori_loop(0, TILES // unroll, merge, start, unroll=4)


def beam_kernel(w_ref, *refs):
    v_refs, out_refs, sums_ref = refs[:STA], refs[STA : 2 * STA], refs[2 * STA]
    w = w_ref[0].astype(f32)
    rows = []
    for d in range(STA):
        w_re = w[0, d * BEAMS : (d + 1) * BEAMS]
        w_im = w[1, d * BEAMS : (d + 1) * BEAMS]
        rows.append(jnp.concatenate([w_re, -w_im], axis=1))
        rows.append(jnp.concatenate([w_im, w_re], axis=1))
    left = jnp.concatenate(rows, axis=0).astype(bf16)
    me = lax.axis_index("sta")
    me_x, me_y = lax.shift_right_logical(me, 2), me & 3
    old = lax.broadcasted_iota(jnp.int32, (128, 128), 0)
    new = lax.broadcasted_iota(jnp.int32, (128, 128), 1)
    group = lax.shift_right_logical(new, 3) & 7
    source = ((me_x + lax.shift_right_logical(group, 2)) & 1) * 4 + ((me_y - group) & 3)
    pick = old == ((new & 64) | (source << 3) | (new & 7))
    left = jnp.dot(left, pick.astype(f32).astype(bf16), preferred_element_type=f32).astype(bf16)
    new = lax.broadcasted_iota(jnp.int32, (64, 64), 0)
    old = lax.broadcasted_iota(jnp.int32, (64, 64), 1)
    group = lax.shift_right_logical(new, 3)
    target = ((me_x + lax.shift_right_logical(group, 2)) & 1) * 4 + ((me_y + group) & 3)
    pick = old == ((target << 3) | (new & 7))
    left = jnp.dot(pick.astype(f32).astype(bf16), left, preferred_element_type=f32).astype(bf16)
    chunk = 1024
    peak = jnp.zeros((64, LANES), f32)
    for i in range(BLOCK // chunk):
        at = slice(i * chunk, (i + 1) * chunk)
        volts = jnp.concatenate([v[0, :, at] for v in v_refs] + [v[1, :, at] for v in v_refs], axis=0)
        sums = jnp.dot(left, volts, preferred_element_type=f32)
        sums_ref[:, at] = sums
        for u in range(chunk // LANES):
            peak = jnp.maximum(peak, jnp.abs(sums[:, u * LANES : (u + 1) * LANES]))
    code = code_of(peak)
    inverse = LEVELS / scale_of(code)
    for d in range(STA):
        at8 = slice(d * 8, d * 8 + 8)
        factor = inverse[at8]
        out_ref = out_refs[d]
        out_ref[:, BLOCK:] = code[at8].astype(jnp.int32).astype(jnp.int16)

        def pack(i, carry):
            at = pl.multiple_of(i * 1024, 1024)
            x = sums_ref[at8, pl.ds(at, 1024)]
            x = x * jnp.concatenate([factor] * 8, axis=1)
            out_ref[:, pl.ds(at, 1024)] = jnp.round(x).astype(jnp.int32).astype(jnp.int16)
            return carry

        lax.fori_loop(0, BLOCK // 1024, pack, 0, unroll=4)


def halves(x, axis):
    high = x.astype(bf16)
    low = (x - high.astype(f32)).astype(bf16)
    return jnp.concatenate([high, low, high], axis=axis)


def dot_left(table_ref, parity, u):
    high, low = table_ref[parity, 0], table_ref[parity, 1]
    return jnp.dot(jnp.concatenate([high, high, low], axis=1), halves(u, 0), preferred_element_type=f32)


def dot_right(u, table_ref, parity):
    high, low = table_ref[parity, 0], table_ref[parity, 1]
    return jnp.dot(halves(u, 1), jnp.concatenate([high, high, low], axis=0), preferred_element_type=f32)


QUARTER_HIGH = 1.5703125
QUARTER_LOW = float(np.float32(np.pi / 2 - QUARTER_HIGH))


def cos_sin(phase):
    turns = jnp.round(phase * (2 / np.pi))
    r = (phase - turns * QUARTER_HIGH) - turns * QUARTER_LOW
    quadrant = turns.astype(jnp.int32)
    z = r * r
    s = r + r * z * (-1.6666654611e-1 + z * (8.3321608736e-3 + z * (-1.9515295891e-4)))
    c = 1.0 - 0.5 * z + z * z * (4.166664568298827e-2 + z * (-1.388731625493765e-3 + z * 2.443315711809948e-5))
    odd = (quadrant & 1) == 1
    cos = jnp.where(odd, s, c)
    sin = jnp.where(odd, c, s)
    cos = jnp.where(((quadrant + 1) & 2) == 2, -cos, cos)
    sin = jnp.where((quadrant & 2) == 2, -sin, sin)
    return cos, sin


def chirp_kernel(dm_ref, after_ref, out_ref):
    centre = BASE_FREQ + CHANNEL_WIDTH * (lax.axis_index("sub").astype(f32) + 0.5)
    row = lax.broadcasted_iota(jnp.int32, (8, ROOT), 0)
    col = lax.broadcasted_iota(jnp.int32, (8, ROOT), 1)
    k2 = ROOT * (2 * (col & (HALF - 1)) + lax.shift_right_logical(col, 7))
    measures = [DM_STEP * dm_ref[b].astype(f32) for b in range(BEAMS)]

    def chirp(i, carry):
        at = pl.ds(pl.multiple_of(i * 8, 8), 8)
        k1 = 2 * ((row + i * 8) & (HALF - 1)) + i // (HALF // 8)
        position = k1 + k2
        signed = jnp.where(position < TOTAL // 2, position, position - TOTAL)
        offset = CHANNEL_WIDTH * signed.astype(f32) / TOTAL
        base = (TWO_PI * DISPERSION) * offset * offset / (centre * centre * (centre + offset))
        for b in range(BEAMS):
            c, s = cos_sin(measures[b] * base)
            out_ref[b, 0, at, :] = c
            out_ref[b, 1, at, :] = s
        return carry

    lax.fori_loop(0, ROOT // 8, chirp, 0, unroll=2)


def dedisperse_kernel(
    chirp_ref, fwd_ref, bwd_ref, end_ref, tw_ref, *refs
):
    x_refs, out_ref, time_ref, last_ref = refs[:STA], refs[STA], refs[STA + 1], refs[STA + 2]
    for x_ref, hop in zip(x_refs, HOPS):
        scale = scale_of(widen(x_ref[:, BLOCK:])) * (1.0 / LEVELS)
        first_tile = neighbour(hop, -1) * TILES

        def decode(i, carry):
            at = pl.multiple_of(i * 512, 512)
            x = widen(x_ref[:, pl.ds(at, 512)])
            for u in range(4):
                time_ref[first_tile + i * 4 + u] = x[:, u * LANES : (u + 1) * LANES] * scale
            return carry

        lax.fori_loop(0, TILES // 4, decode, 0, unroll=4)

    flat = time_ref.reshape(TOTAL // LANES * 8, LANES)
    def beam(b):
        x = []
        for p in range(2):
            x.append(
                jnp.concatenate([flat[pl.ds(h * 8 + p * 4 + b, ROOT, stride=16), :] for h in range(2)], axis=1)
            )
        yield
        outs = []
        for parity in range(2):
            u = [v[:HALF] + v[HALF:] if parity == 0 else v[:HALF] - v[HALF:] for v in x]
            u = jnp.concatenate(u, axis=0)
            outs.append(dot_left(fwd_ref, parity, u))
        yield
        re = jnp.concatenate([o[:HALF] for o in outs], axis=0)
        im = jnp.concatenate([o[HALF:] for o in outs], axis=0)
        tw_re, tw_im = tw_ref[0], tw_ref[1]
        re, im = re * tw_re + im * tw_im, im * tw_re - re * tw_im
        outs = []
        for parity in range(2):
            u = [v[:, :HALF] + v[:, HALF:] if parity == 0 else v[:, :HALF] - v[:, HALF:] for v in (re, im)]
            u = jnp.concatenate(u, axis=1)
            outs.append(dot_right(u, bwd_ref, parity))
        yield
        sums = []
        for parity in range(2):
            at = slice(parity * HALF, (parity + 1) * HALF)
            c, s = chirp_ref[b, 0, :, at], chirp_ref[b, 1, :, at]
            y_re, y_im = outs[parity][:, :HALF], outs[parity][:, HALF:]
            u = jnp.concatenate([y_re * c - y_im * s, y_re * s + y_im * c], axis=1)
            sums.append(dot_right(u, fwd_ref, parity))
        yield
        top, bottom = sums[0] + sums[1], sums[0] - sums[1]
        re = jnp.concatenate([top[:, :HALF], bottom[:, :HALF]], axis=1)
        im = jnp.concatenate([top[:, HALF:], bottom[:, HALF:]], axis=1)
        re, im = re * tw_re - im * tw_im, im * tw_re + re * tw_im
        sums = []
        for parity in range(2):
            at = slice(parity * HALF, (parity + 1) * HALF)
            u = jnp.concatenate([re[at], im[at]], axis=0)
            sums.append(dot_left(end_ref, parity, u))
        yield
        top, bottom = sums[0] + sums[1], sums[0] - sums[1]
        for p in range(2):
            for r in range(2):
                at = slice(p * HALF + r * 64, p * HALF + r * 64 + 64)
                for h in range(2):
                    lanes = slice(h * LANES, (h + 1) * LANES)
                    first = b * 4 + r * 2 + h
                    last_ref[p, first, :64] = top[at, lanes]
                    last_ref[p, first, 64:] = bottom[at, lanes]

    running = [beam(b) for b in range(BEAMS)]
    for tick in range(1 * (BEAMS - 1) + 6):
        for b in range(BEAMS):
            if tick >= 1 * b:
                next(running[b], None)

    def encode(i, carry):
        at = pl.ds(pl.multiple_of(i * 8, 8), 8)
        x = [[last_ref[p, k, at, :] for k in range(16)] for p in range(2)]
        peak = jnp.abs(x[0][0])
        for k in range(1, 32):
            peak = jnp.maximum(peak, jnp.abs(x[k // 16][k % 16]))
        code = code_of(peak)
        inverse = LEVELS / scale_of(code)
        first = i * (8 * ROWS)
        for k in range(16):
            low = jnp.round(x[0][k] * inverse).astype(jnp.int32) & 0xFFFF
            high = jnp.round(x[1][k] * inverse).astype(jnp.int32) << 16
            out_ref[pl.ds(first + k, 8, stride=ROWS), :] = low | high
        out_ref[pl.ds(first + 16, 8, stride=ROWS), :] = code.astype(jnp.int32)
        return carry

    lax.fori_loop(0, DEVICES // 8, encode, 0, unroll=2)


SUBS = 4


def finish_kernel(x_ref, out_ref, power_ref):
    step = pl.program_id(0)

    @pl.when(step == 0)
    def _():
        power_ref[...] = jnp.zeros_like(power_ref)

    scales = []
    for sub in range(SUBS):
        code = x_ref[pl.ds(sub * STA * ROWS + 16, STA, stride=ROWS), :]
        scales.append(scale_of(code.astype(f32)) * (1.0 / LEVELS))
    for sta in range(STA):
        power = power_ref[sta * 16 : sta * 16 + 16, :]
        for sub in range(SUBS):
            src = (sub * STA + sta) * ROWS
            to = sub * 256 + sta * 16
            scale = jnp.broadcast_to(scales[sub][sta : sta + 1], (16, LANES))
            both = x_ref[src : src + 16, :]
            re = ((both << 16) >> 16).astype(f32) * scale
            im = (both >> 16).astype(f32) * scale
            out_ref[to : to + 16, :] = re
            out_ref[to + 128 : to + 144, :] = im
            power = power + (re * re + im * im)
        power_ref[sta * 16 : sta * 16 + 16, :] = power

    @pl.when(step == pl.num_programs(0) - 1)
    def _():
        power_ref[...] = power_ref[...] * (1.0 / 16.0)


VMEM = pl.BlockSpec(memory_space=pltpu.VMEM)
SMEM = pl.BlockSpec(memory_space=pltpu.SMEM)
HBM = pl.BlockSpec(memory_space=pltpu.HBM)
PARAMS = pltpu.CompilerParams(vmem_limit_bytes=36 * 1024 * 1024)


SHIFT_PARAMS = pltpu.CompilerParams(vmem_limit_bytes=50 * 1024 * 1024 + 512 * 1024)


def shift(voltages, delays):
    return pl.pallas_call(
        shift_kernel,
        out_shape=[jax.ShapeDtypeStruct((2, STA, BLOCK), bf16)] * STA,
        in_specs=[HBM, HBM],
        out_specs=[VMEM] * STA,
        scratch_shapes=[
            pltpu.VMEM((2, STA, TOTAL), bf16),
            pltpu.SMEM((STA,), jnp.int32),
            pltpu.VMEM((2, (TOTAL // LANES + FRONT) * STA, LANES), f32),
            pltpu.VMEM((2, (TOTAL // LANES + 8) * STA, LANES), f32),
            pltpu.SemaphoreType.DMA((5,)),
        ],
        compiler_params=SHIFT_PARAMS,
        name="shift",
    )(delays, voltages)


def beamform(volts, weights):
    return pl.pallas_call(
        beam_kernel,
        out_shape=[jax.ShapeDtypeStruct((8, BLOCK + LANES), jnp.int16)] * STA,
        in_specs=[VMEM] * (1 + STA),
        out_specs=[VMEM] * STA,
        scratch_shapes=[pltpu.VMEM((64, BLOCK), f32)],
        compiler_params=PARAMS,
        name="beamform",
    )(weights, *volts)


def chirps(dm_index, after):
    return pl.pallas_call(
        chirp_kernel,
        out_shape=jax.ShapeDtypeStruct((BEAMS, 2, ROOT, ROOT), f32),
        in_specs=[SMEM, HBM],
        out_specs=VMEM,
        compiler_params=PARAMS,
        cost_estimate=pl.CostEstimate(flops=20_000_000, transcendentals=0, bytes_accessed=2 << 20),
        name="chirps",
    )(dm_index, after)


def dedisperse(chirp, coded):
    fwd, bwd, end, tw = tables()
    return pl.pallas_call(
        dedisperse_kernel,
        out_shape=jax.ShapeDtypeStruct((DEVICES * ROWS, LANES), jnp.int32),
        in_specs=[VMEM] * (5 + STA),
        out_specs=VMEM,
        scratch_shapes=[
            pltpu.VMEM((TOTAL // LANES, 8, LANES), f32),
            pltpu.VMEM((2, 16, DEVICES, LANES), f32),
        ],
        compiler_params=PARAMS,
        name="dedisperse",
    )(chirp, fwd, bwd, end, tw, *coded)


def finish(coded):
    return pl.pallas_call(
        finish_kernel,
        grid=(16 // SUBS,),
        out_shape=(jax.ShapeDtypeStruct((4096, LANES), f32), jax.ShapeDtypeStruct((128, LANES), f32)),
        in_specs=[pl.BlockSpec((SUBS * STA * ROWS, LANES), lambda s: (s, 0))],
        out_specs=(
            pl.BlockSpec((SUBS * 256, LANES), lambda s: (s, 0)),
            pl.BlockSpec((128, LANES), lambda s: (0, 0)),
        ),
        compiler_params=PARAMS,
        name="finish",
    )(coded)


def exchange(blocks):
    received = [blocks[0]]
    for block, hop in zip(blocks[1:], HOPS[1:]):
        pairs = [(x * 4 + y, (x + hop[0]) % 2 * 4 + (y + hop[1]) % 4) for x in range(2) for y in range(4)]
        received.append(lax.ppermute(block, "sta", pairs))
    return received


def shards(voltages, beam_weights, station_delays, dm_index):
    blocks = shift(voltages, station_delays)
    chirp = chirps(dm_index.reshape(BEAMS), blocks[0])
    coded = exchange(beamform(exchange(blocks), beam_weights))
    coded = dedisperse(chirp, coded).reshape(DEVICES, 1, ROWS * LANES)
    coded = lax.all_to_all(coded, ("sub", "sta"), 0, 0, tiled=True).reshape(DEVICES * ROWS, LANES)
    moved, intensity = finish(coded)
    return moved.reshape(16, 2, 32, 1, 512), intensity.reshape(32, 1, 512)


def solution(mesh):
    return jax.shard_map(
        shards,
        mesh=mesh,
        in_specs=(
            P("sub", None, "sta", None),
            P("sub", None, None, None),
            P("sta"),
            P("sta", None),
        ),
        out_specs=(P(None, None, None, None, ("sub", "sta")), P(None, None, ("sub", "sta"))),
        check_vma=False,
    )
```

```python
import functools

import jax
import jax.numpy as jnp
import numpy as np
from jax import lax
from jax.experimental import pallas as pl
from jax.experimental.pallas import tpu as pltpu
from jax.sharding import PartitionSpec as P

TWO_PI = 6.283185307179586
DISPERSION = 4148808000.0
DM_STEP = 10.0
BASE_FREQ = 120.0
CHANNEL_WIDTH = 0.1953125

TOTAL = 65536
ROOT = 256
HALF = 128
LANES = 128
STA = 8
BLOCK = TOTAL // STA
TILES = BLOCK // LANES
BEAMS = 4
DEVICES = 128
ROWS = 17
CODE_STEP = 64.0
LEVELS = 32767.0
FLOOR = 1e-33

HOPS = [(0, 0), (1, 0), (0, 2), (1, 2), (0, 1), (1, 1), (0, 3), (1, 3)]


f32 = jnp.float32
bf16 = jnp.bfloat16


def neighbour(hop, sign):
    me = lax.axis_index("sta")
    x = (lax.shift_right_logical(me, 2) + hop[0]) & 1
    y = ((me & 3) + sign * hop[1]) & 3
    return x * 4 + y


def split_np(table):
    high = table.astype(bf16)
    low = (table - high.astype(np.float64)).astype(bf16)
    return high, low


@functools.lru_cache(maxsize=None)
def tables():
    m = np.arange(HALF)
    fwd = []
    for parity in range(2):
        angle = 2 * np.pi * (((2 * m[:, None] + parity) * m[None, :]) % ROOT) / ROOT
        c, s = np.cos(angle), np.sin(angle)
        fwd.append(np.block([[c, s], [-s, c]]))
    fwd = np.stack(fwd)
    bwd = fwd.transpose(0, 2, 1)
    order = (2 * np.arange(64)[None, :] + np.arange(2)[:, None]).reshape(-1)
    order = np.concatenate([order, HALF + order])
    last = bwd[:, order, :] / TOTAL

    def pair(t):
        return np.stack(split_np(t), axis=1)

    rows = np.concatenate([2 * m, 2 * m + 1])
    angle = 2 * np.pi * (rows[:, None] * np.arange(ROOT)[None, :]) / TOTAL
    twiddle = np.stack([np.cos(angle), np.sin(angle)]).astype(np.float32)
    return pair(fwd), pair(bwd), pair(last), twiddle


def code_of(peak):
    return jnp.ceil(jnp.log(jnp.maximum(peak, FLOOR)) * (CODE_STEP / 0.6931471805599453)) + 1.0


def scale_of(code):
    return jnp.exp2(code * (1.0 / CODE_STEP))


def quantize(x, inverse):
    return jnp.round(x * inverse).astype(jnp.int32).astype(jnp.int16)


def widen(q):
    return q.astype(jnp.int32).astype(f32)


FRONT = 136


def shift_kernel(delay_hbm, v_hbm, *refs):
    out_refs = refs[:STA]
    v_ref, delay_ref, plain_ref, turned_ref, sems = refs[STA:]
    halves_at = [pl.ds(h * (TOTAL // 2), TOTAL // 2) for h in range(2)]
    delays = pltpu.make_async_copy(delay_hbm, delay_ref, sems.at[4])
    delays.start()
    copies = []
    for p in range(2):
        for h in range(2):
            source, to = v_hbm.at[0, p, :, halves_at[h]], v_ref.at[p, :, halves_at[h]]
            copies.append(pltpu.make_async_copy(source, to, sems.at[p * 2 + h]))
            copies[-1].start()
    delays.wait()
    count = TOTAL // LANES
    lane = lax.broadcasted_iota(jnp.int32, (STA, LANES), 1)
    row = lax.broadcasted_iota(jnp.int32, (STA, LANES), 0)
    fine = jnp.zeros((STA, LANES), jnp.int32)
    for q in range(STA):
        fine = jnp.where(row == q, delay_ref[q] & (LANES - 1), fine)
    keep = lane >= fine
    source = lax.broadcasted_iota(jnp.int32, (LANES, LANES), 0)
    target = lax.broadcasted_iota(jnp.int32, (LANES, LANES), 1)
    turn = (target - source) & (LANES - 1)
    none = jnp.zeros((LANES, LANES), bf16)
    matrices = []
    for q in range(0, STA, 2):
        pair = [(turn == (delay_ref[q + i] & (LANES - 1))).astype(f32).astype(bf16) for i in range(2)]
        top = jnp.concatenate([pair[0], none], axis=1)
        low = jnp.concatenate([none, pair[1]], axis=1)
        matrices.append(jnp.concatenate([top, low], axis=0))
    unroll = 8
    rows = count + 8
    steps = count // unroll
    for p in range(2):
        plain = plain_ref.at[p]

        def fill(i, carry):
            at = pl.multiple_of(i * (unroll * LANES), unroll * LANES)
            x = v_ref[p, :, pl.ds(at, unroll * LANES)].astype(f32)
            for u in range(unroll):
                to = pl.multiple_of((FRONT + i * unroll + u) * STA, STA)
                plain[pl.ds(to, STA), :] = x[:, u * LANES : (u + 1) * LANES]
            return carry

        def wrap(i, carry):
            at = pl.multiple_of((TOTAL - FRONT * LANES) + i * (unroll * LANES), unroll * LANES)
            x = v_ref[p, :, pl.ds(at, unroll * LANES)].astype(f32)
            for u in range(unroll):
                to = pl.multiple_of((i * unroll + u) * STA, STA)
                plain[pl.ds(to, STA), :] = x[:, u * LANES : (u + 1) * LANES]
            return carry

        for h in range(2):
            copies[p * 2 + h].wait()
            lax.fori_loop(h * steps // 2, (h + 1) * steps // 2, fill, 0, unroll=4)
        lax.fori_loop(0, FRONT // unroll, wrap, 0, unroll=2)
    for q in range(0, STA, 2):
        for p in range(2):
            x = []
            for i in range(2):
                coarse = lax.shift_right_logical(delay_ref[q + i], 7)
                first = (FRONT - 8 - coarse) * STA + q + i
                x.append(plain_ref.at[p][pl.ds(first, rows, stride=STA), :].astype(bf16))
            y = jnp.dot(jnp.concatenate(x, axis=1), matrices[q // 2], preferred_element_type=f32)
            for i in range(2):
                turned_ref.at[p][pl.ds(q + i, rows, stride=STA), :] = y[:, i * LANES : (i + 1) * LANES]

    for out_ref, hop in zip(out_refs, HOPS):
        first = neighbour(hop, 1) * TILES

        def merge(i, before):
            at = pl.multiple_of(i * (unroll * LANES), unroll * LANES)
            last = []
            for p in range(2):
                parts = []
                old = before[p]
                for u in range(unroll):
                    tile = 8 + first + i * unroll + u
                    now = turned_ref[p, pl.ds(pl.multiple_of(tile * STA, STA), STA), :]
                    parts.append(jnp.where(keep, now, old))
                    old = now
                out_ref[p, :, pl.ds(at, unroll * LANES)] = jnp.concatenate(parts, axis=1).astype(bf16)
                last.append(old)
            return tuple(last)

        start = tuple(turned_ref[p, pl.ds(pl.multiple_of((7 + first) * STA, STA), STA), :] for p in range(2))
        lax.fori_loop(0, TILES // unroll, merge, start, unroll=4)


def beam_kernel(w_ref, after_ref, *refs):
    v_refs, out_refs, sums_ref = refs[:STA], refs[STA : 2 * STA], refs[2 * STA]
    w = w_ref[0].astype(f32)
    rows = []
    for d in range(STA):
        w_re = w[0, d * BEAMS : (d + 1) * BEAMS]
        w_im = w[1, d * BEAMS : (d + 1) * BEAMS]
        rows.append(jnp.concatenate([w_re, -w_im], axis=1))
        rows.append(jnp.concatenate([w_im, w_re], axis=1))
    left = jnp.concatenate(rows, axis=0).astype(bf16)
    old = lax.broadcasted_iota(jnp.int32, (128, 128), 0)
    new = lax.broadcasted_iota(jnp.int32, (128, 128), 1)
    group = lax.shift_right_logical(new, 3) & 7
    wanted = (new & 64) | (new & 7)
    for r, hop in enumerate(HOPS):
        wanted = jnp.where(group == r, wanted + neighbour(hop, -1) * 8, wanted)
    left = jnp.dot(left, (old == wanted).astype(f32).astype(bf16), preferred_element_type=f32).astype(bf16)
    new = lax.broadcasted_iota(jnp.int32, (64, 64), 0)
    old = lax.broadcasted_iota(jnp.int32, (64, 64), 1)
    group = lax.shift_right_logical(new, 3)
    wanted = new & 7
    for r, hop in enumerate(HOPS):
        wanted = jnp.where(group == r, wanted + neighbour(hop, 1) * 8, wanted)
    left = jnp.dot((old == wanted).astype(f32).astype(bf16), left, preferred_element_type=f32).astype(bf16)
    chunk = 1024
    peak = jnp.zeros((64, LANES), f32)
    for i in range(BLOCK // chunk):
        at = slice(i * chunk, (i + 1) * chunk)
        volts = jnp.concatenate([v[0, :, at] for v in v_refs] + [v[1, :, at] for v in v_refs], axis=0)
        sums = jnp.dot(left, volts, preferred_element_type=f32)
        sums_ref[:, at] = sums
        for u in range(chunk // LANES):
            peak = jnp.maximum(peak, jnp.abs(sums[:, u * LANES : (u + 1) * LANES]))
    code = code_of(peak)
    inverse = LEVELS / scale_of(code)
    for d in range(STA):
        at8 = slice(d * 8, d * 8 + 8)
        factor = inverse[at8]
        out_ref = out_refs[d]
        out_ref[:, BLOCK:] = code[at8].astype(jnp.int32).astype(jnp.int16)

        def pack(i, carry):
            at = pl.multiple_of(i * 1024, 1024)
            x = sums_ref[at8, pl.ds(at, 1024)]
            x = x * jnp.concatenate([factor] * 8, axis=1)
            out_ref[:, pl.ds(at, 1024)] = jnp.round(x).astype(jnp.int32).astype(jnp.int16)
            return carry

        lax.fori_loop(0, BLOCK // 1024, pack, 0, unroll=4)


def halves(x, axis):
    high = x.astype(bf16)
    low = (x - high.astype(f32)).astype(bf16)
    return jnp.concatenate([high, low, high], axis=axis)


def dot_left(table_ref, parity, u):
    high, low = table_ref[parity, 0], table_ref[parity, 1]
    return jnp.dot(jnp.concatenate([high, high, low], axis=1), halves(u, 0), preferred_element_type=f32)


def dot_right(u, table_ref, parity):
    high, low = table_ref[parity, 0], table_ref[parity, 1]
    return jnp.dot(halves(u, 1), jnp.concatenate([high, high, low], axis=0), preferred_element_type=f32)


QUARTER_HIGH = 1.5703125
QUARTER_LOW = float(np.float32(np.pi / 2 - QUARTER_HIGH))


def cos_sin(phase):
    turns = jnp.round(phase * (2 / np.pi))
    r = (phase - turns * QUARTER_HIGH) - turns * QUARTER_LOW
    quadrant = turns.astype(jnp.int32)
    z = r * r
    s = r + r * z * (-1.6666654611e-1 + z * (8.3321608736e-3 + z * (-1.9515295891e-4)))
    c = 1.0 - 0.5 * z + z * z * (4.166664568298827e-2 + z * (-1.388731625493765e-3 + z * 2.443315711809948e-5))
    odd = (quadrant & 1) == 1
    cos = jnp.where(odd, s, c)
    sin = jnp.where(odd, c, s)
    cos = jnp.where(((quadrant + 1) & 2) == 2, -cos, cos)
    sin = jnp.where((quadrant & 2) == 2, -sin, sin)
    return cos, sin


def chirp_kernel(dm_ref, after_ref, out_ref):
    centre = BASE_FREQ + CHANNEL_WIDTH * (lax.axis_index("sub").astype(f32) + 0.5)
    row = lax.broadcasted_iota(jnp.int32, (8, ROOT), 0)
    col = lax.broadcasted_iota(jnp.int32, (8, ROOT), 1)
    k2 = ROOT * (2 * (col & (HALF - 1)) + lax.shift_right_logical(col, 7))
    measures = [DM_STEP * dm_ref[b].astype(f32) for b in range(BEAMS)]

    def chirp(i, carry):
        at = pl.ds(pl.multiple_of(i * 8, 8), 8)
        k1 = 2 * ((row + i * 8) & (HALF - 1)) + i // (HALF // 8)
        position = k1 + k2
        signed = jnp.where(position < TOTAL // 2, position, position - TOTAL)
        offset = CHANNEL_WIDTH * signed.astype(f32) / TOTAL
        base = (TWO_PI * DISPERSION) * offset * offset / (centre * centre * (centre + offset))
        for b in range(BEAMS):
            c, s = cos_sin(measures[b] * base)
            out_ref[b, 0, at, :] = c
            out_ref[b, 1, at, :] = s
        return carry

    lax.fori_loop(0, ROOT // 8, chirp, 0, unroll=2)


def dedisperse_kernel(
    chirp_ref, fwd_ref, bwd_ref, end_ref, tw_ref, *refs
):
    x_refs, out_ref, time_ref, last_ref = refs[:STA], refs[STA], refs[STA + 1], refs[STA + 2]
    for x_ref, hop in zip(x_refs, HOPS):
        scale = scale_of(widen(x_ref[:, BLOCK:])) * (1.0 / LEVELS)
        first_tile = neighbour(hop, -1) * TILES

        def decode(i, carry):
            at = pl.multiple_of(i * 512, 512)
            x = widen(x_ref[:, pl.ds(at, 512)])
            for u in range(4):
                time_ref[first_tile + i * 4 + u] = x[:, u * LANES : (u + 1) * LANES] * scale
            return carry

        lax.fori_loop(0, TILES // 4, decode, 0, unroll=4)

    flat = time_ref.reshape(TOTAL // LANES * 8, LANES)
    def beam(b):
        x = []
        for p in range(2):
            x.append(
                jnp.concatenate([flat[pl.ds(h * 8 + p * 4 + b, ROOT, stride=16), :] for h in range(2)], axis=1)
            )
        yield
        outs = []
        for parity in range(2):
            u = [v[:HALF] + v[HALF:] if parity == 0 else v[:HALF] - v[HALF:] for v in x]
            u = jnp.concatenate(u, axis=0)
            outs.append(dot_left(fwd_ref, parity, u))
        yield
        re = jnp.concatenate([o[:HALF] for o in outs], axis=0)
        im = jnp.concatenate([o[HALF:] for o in outs], axis=0)
        tw_re, tw_im = tw_ref[0], tw_ref[1]
        re, im = re * tw_re + im * tw_im, im * tw_re - re * tw_im
        outs = []
        for parity in range(2):
            u = [v[:, :HALF] + v[:, HALF:] if parity == 0 else v[:, :HALF] - v[:, HALF:] for v in (re, im)]
            u = jnp.concatenate(u, axis=1)
            outs.append(dot_right(u, bwd_ref, parity))
        yield
        sums = []
        for parity in range(2):
            at = slice(parity * HALF, (parity + 1) * HALF)
            c, s = chirp_ref[b, 0, :, at], chirp_ref[b, 1, :, at]
            y_re, y_im = outs[parity][:, :HALF], outs[parity][:, HALF:]
            u = jnp.concatenate([y_re * c - y_im * s, y_re * s + y_im * c], axis=1)
            sums.append(dot_right(u, fwd_ref, parity))
        yield
        top, bottom = sums[0] + sums[1], sums[0] - sums[1]
        re = jnp.concatenate([top[:, :HALF], bottom[:, :HALF]], axis=1)
        im = jnp.concatenate([top[:, HALF:], bottom[:, HALF:]], axis=1)
        re, im = re * tw_re - im * tw_im, im * tw_re + re * tw_im
        sums = []
        for parity in range(2):
            at = slice(parity * HALF, (parity + 1) * HALF)
            u = jnp.concatenate([re[at], im[at]], axis=0)
            sums.append(dot_left(end_ref, parity, u))
        yield
        top, bottom = sums[0] + sums[1], sums[0] - sums[1]
        for p in range(2):
            for r in range(2):
                at = slice(p * HALF + r * 64, p * HALF + r * 64 + 64)
                for h in range(2):
                    lanes = slice(h * LANES, (h + 1) * LANES)
                    first = b * 4 + r * 2 + h
                    last_ref[p, first, :64] = top[at, lanes]
                    last_ref[p, first, 64:] = bottom[at, lanes]

    running = [beam(b) for b in range(BEAMS)]
    for tick in range(1 * (BEAMS - 1) + 6):
        for b in range(BEAMS):
            if tick >= 1 * b:
                next(running[b], None)

    def encode(i, carry):
        at = pl.ds(pl.multiple_of(i * 8, 8), 8)
        x = [[last_ref[p, k, at, :] for k in range(16)] for p in range(2)]
        peak = jnp.abs(x[0][0])
        for k in range(1, 32):
            peak = jnp.maximum(peak, jnp.abs(x[k // 16][k % 16]))
        code = code_of(peak)
        inverse = LEVELS / scale_of(code)
        first = i * (8 * ROWS)
        for k in range(16):
            low = jnp.round(x[0][k] * inverse).astype(jnp.int32) & 0xFFFF
            high = jnp.round(x[1][k] * inverse).astype(jnp.int32) << 16
            out_ref[pl.ds(first + k, 8, stride=ROWS), :] = low | high
        out_ref[pl.ds(first + 16, 8, stride=ROWS), :] = code.astype(jnp.int32)
        return carry

    lax.fori_loop(0, DEVICES // 8, encode, 0, unroll=2)


def finish_kernel(x_ref, out_hbm, power_ref, out_ref, sems):
    copies = []
    for sub in range(16):
        code = x_ref[pl.ds(sub * STA * ROWS + 16, STA, stride=ROWS), :]
        scales = scale_of(code.astype(f32)) * (1.0 / LEVELS)
        for sta in range(STA):
            src = (sub * STA + sta) * ROWS
            to = sub * 256 + sta * 16
            scale = jnp.broadcast_to(scales[sta : sta + 1], (16, LANES))
            both = x_ref[src : src + 16, :]
            out_ref[to : to + 16, :] = ((both << 16) >> 16).astype(f32) * scale
            out_ref[to + 128 : to + 144, :] = (both >> 16).astype(f32) * scale
        rows = pl.ds(sub * 256, 256)
        copies.append(pltpu.make_async_copy(out_ref.at[rows], out_hbm.at[rows], sems.at[sub]))
        copies[-1].start()
    for i in range(16):
        power = jnp.zeros((8, LANES), f32)
        for sub in range(16):
            re = out_ref[sub * 256 + i * 8 : sub * 256 + i * 8 + 8, :]
            im = out_ref[sub * 256 + 128 + i * 8 : sub * 256 + 136 + i * 8, :]
            power = power + (re * re + im * im)
        power_ref[i * 8 : i * 8 + 8, :] = power * (1.0 / 16.0)
    for copy in copies:
        copy.wait()


VMEM = pl.BlockSpec(memory_space=pltpu.VMEM)
SMEM = pl.BlockSpec(memory_space=pltpu.SMEM)
HBM = pl.BlockSpec(memory_space=pltpu.HBM)
PARAMS = pltpu.CompilerParams(vmem_limit_bytes=36 * 1024 * 1024)


SHIFT_PARAMS = pltpu.CompilerParams(vmem_limit_bytes=50 * 1024 * 1024 + 512 * 1024)


def shift(voltages, delays):
    return pl.pallas_call(
        shift_kernel,
        out_shape=[jax.ShapeDtypeStruct((2, STA, BLOCK), bf16)] * STA,
        in_specs=[HBM, HBM],
        out_specs=[VMEM] * STA,
        scratch_shapes=[
            pltpu.VMEM((2, STA, TOTAL), bf16),
            pltpu.SMEM((STA,), jnp.int32),
            pltpu.VMEM((2, (TOTAL // LANES + FRONT) * STA, LANES), f32),
            pltpu.VMEM((2, (TOTAL // LANES + 8) * STA, LANES), f32),
            pltpu.SemaphoreType.DMA((5,)),
        ],
        compiler_params=SHIFT_PARAMS,
        name="shift",
    )(delays, voltages)


def beamform(volts, weights, after):
    return pl.pallas_call(
        beam_kernel,
        out_shape=[jax.ShapeDtypeStruct((8, BLOCK + LANES), jnp.int16)] * STA,
        in_specs=[VMEM, HBM] + [VMEM] * STA,
        out_specs=[VMEM] * STA,
        scratch_shapes=[pltpu.VMEM((64, BLOCK), f32)],
        compiler_params=PARAMS,
        name="beamform",
    )(weights, after, *volts)


def chirps(dm_index, after):
    return pl.pallas_call(
        chirp_kernel,
        out_shape=jax.ShapeDtypeStruct((BEAMS, 2, ROOT, ROOT), f32),
        in_specs=[SMEM, HBM],
        out_specs=VMEM,
        compiler_params=PARAMS,
        cost_estimate=pl.CostEstimate(flops=20_000_000, transcendentals=0, bytes_accessed=2 << 20),
        name="chirps",
    )(dm_index, after)


def dedisperse(chirp, coded):
    fwd, bwd, end, tw = tables()
    return pl.pallas_call(
        dedisperse_kernel,
        out_shape=jax.ShapeDtypeStruct((DEVICES * ROWS, LANES), jnp.int32),
        in_specs=[VMEM] * (5 + STA),
        out_specs=VMEM,
        scratch_shapes=[
            pltpu.VMEM((TOTAL // LANES, 8, LANES), f32),
            pltpu.VMEM((2, 16, DEVICES, LANES), f32),
        ],
        compiler_params=PARAMS,
        name="dedisperse",
    )(chirp, fwd, bwd, end, tw, *coded)


def finish(coded):
    return pl.pallas_call(
        finish_kernel,
        out_shape=(jax.ShapeDtypeStruct((4096, LANES), f32), jax.ShapeDtypeStruct((128, LANES), f32)),
        in_specs=[VMEM],
        out_specs=(HBM, VMEM),
        scratch_shapes=[pltpu.VMEM((4096, LANES), f32), pltpu.SemaphoreType.DMA((16,))],
        compiler_params=PARAMS,
        name="finish",
    )(coded)


def exchange(blocks):
    received = [blocks[0]]
    for block, hop in zip(blocks[1:], HOPS[1:]):
        pairs = [(x * 4 + y, (x + hop[0]) % 2 * 4 + (y + hop[1]) % 4) for x in range(2) for y in range(4)]
        received.append(lax.ppermute(block, "sta", pairs))
    return received


def shards(voltages, beam_weights, station_delays, dm_index):
    blocks = shift(voltages, station_delays)
    chirp = chirps(dm_index.reshape(BEAMS), blocks[0])
    coded = exchange(beamform(exchange(blocks), beam_weights, chirp))
    coded = dedisperse(chirp, coded).reshape(DEVICES, 1, ROWS * LANES)
    coded = lax.all_to_all(coded, ("sub", "sta"), 0, 0, tiled=True).reshape(DEVICES * ROWS, LANES)
    moved, intensity = finish(coded)
    return moved.reshape(16, 2, 32, 1, 512), intensity.reshape(32, 1, 512)


def solution(mesh):
    return jax.shard_map(
        shards,
        mesh=mesh,
        in_specs=(
            P("sub", None, "sta", None),
            P("sub", None, None, None),
            P("sta"),
            P("sta", None),
        ),
        out_specs=(P(None, None, None, None, ("sub", "sta")), P(None, None, ("sub", "sta"))),
        check_vma=False,
    )
```

```python
import functools

import jax
import jax.numpy as jnp
import numpy as np
from jax import lax
from jax.experimental import pallas as pl
from jax.experimental.pallas import tpu as pltpu
from jax.sharding import PartitionSpec as P

TWO_PI = 6.283185307179586
DISPERSION = 4148808000.0
DM_STEP = 10.0
BASE_FREQ = 120.0
CHANNEL_WIDTH = 0.1953125

TOTAL = 65536
ROOT = 256
HALF = 128
LANES = 128
STA = 8
BLOCK = TOTAL // STA
TILES = BLOCK // LANES
BEAMS = 4
DEVICES = 128
ROWS = 17
CODE_STEP = 64.0
LEVELS = 32767.0
FLOOR = 1e-33

HOPS = [(0, 0), (1, 0), (0, 2), (1, 2), (0, 1), (1, 1), (0, 3), (1, 3)]


f32 = jnp.float32
bf16 = jnp.bfloat16


def neighbour(hop, sign):
    me = lax.axis_index("sta")
    x = (lax.shift_right_logical(me, 2) + hop[0]) & 1
    y = ((me & 3) + sign * hop[1]) & 3
    return x * 4 + y


def split_np(table):
    high = table.astype(bf16)
    low = (table - high.astype(np.float64)).astype(bf16)
    return high, low


@functools.lru_cache(maxsize=None)
def tables():
    m = np.arange(HALF)
    fwd = []
    for parity in range(2):
        angle = 2 * np.pi * (((2 * m[:, None] + parity) * m[None, :]) % ROOT) / ROOT
        c, s = np.cos(angle), np.sin(angle)
        fwd.append(np.block([[c, s], [-s, c]]))
    fwd = np.stack(fwd)
    bwd = fwd.transpose(0, 2, 1)
    order = (2 * np.arange(64)[None, :] + np.arange(2)[:, None]).reshape(-1)
    order = np.concatenate([order, HALF + order])
    last = bwd[:, order, :] / TOTAL

    def pair(t):
        return np.stack(split_np(t), axis=1)

    rows = np.concatenate([2 * m, 2 * m + 1])
    angle = 2 * np.pi * (rows[:, None] * np.arange(ROOT)[None, :]) / TOTAL
    twiddle = np.stack([np.cos(angle), np.sin(angle)]).astype(np.float32)
    return pair(fwd), pair(bwd), pair(last), twiddle


def code_of(peak):
    return jnp.ceil(jnp.log(jnp.maximum(peak, FLOOR)) * (CODE_STEP / 0.6931471805599453)) + 1.0


def scale_of(code):
    return jnp.exp2(code * (1.0 / CODE_STEP))


def quantize(x, inverse):
    return jnp.round(x * inverse).astype(jnp.int32).astype(jnp.int16)


def widen(q):
    return q.astype(jnp.int32).astype(f32)


PITCH = 9
FRONT = 136


def shift_kernel(delay_hbm, v_hbm, *refs):
    out_refs = refs[:STA]
    v_ref, delay_ref, plain_ref, turned_ref, sems = refs[STA:]
    halves_at = [pl.ds(h * (TOTAL // 2), TOTAL // 2) for h in range(2)]
    delays = pltpu.make_async_copy(delay_hbm, delay_ref, sems.at[4])
    delays.start()
    copies = []
    for p in range(2):
        for h in range(2):
            source, to = v_hbm.at[0, p, :, halves_at[h]], v_ref.at[p, :, halves_at[h]]
            copies.append(pltpu.make_async_copy(source, to, sems.at[p * 2 + h]))
            copies[-1].start()
    delays.wait()
    count = TOTAL // LANES
    lane = lax.broadcasted_iota(jnp.int32, (STA, LANES), 1)
    row = lax.broadcasted_iota(jnp.int32, (STA, LANES), 0)
    fine = jnp.zeros((STA, LANES), jnp.int32)
    for q in range(STA):
        fine = jnp.where(row == q, delay_ref[q] & (LANES - 1), fine)
    keep = lane >= fine
    source = lax.broadcasted_iota(jnp.int32, (LANES, LANES), 0)
    target = lax.broadcasted_iota(jnp.int32, (LANES, LANES), 1)
    turn = (target - source) & (LANES - 1)
    none = jnp.zeros((LANES, LANES), bf16)
    matrices = []
    for q in range(0, STA, 2):
        pair = [(turn == (delay_ref[q + i] & (LANES - 1))).astype(f32).astype(bf16) for i in range(2)]
        top = jnp.concatenate([pair[0], none], axis=1)
        low = jnp.concatenate([none, pair[1]], axis=1)
        matrices.append(jnp.concatenate([top, low], axis=0))
    unroll = 8
    rows = count + 8
    steps = count // unroll
    for p in range(2):
        plain = plain_ref.at[p]

        def fill(i, carry):
            at = pl.multiple_of(i * (unroll * LANES), unroll * LANES)
            x = v_ref[p, :, pl.ds(at, unroll * LANES)].astype(f32)
            for u in range(unroll):
                to = (FRONT + i * unroll + u) * PITCH
                plain[pl.ds(to, STA), :] = x[:, u * LANES : (u + 1) * LANES]
            return carry

        def wrap(i, carry):
            at = pl.multiple_of((TOTAL - FRONT * LANES) + i * (unroll * LANES), unroll * LANES)
            x = v_ref[p, :, pl.ds(at, unroll * LANES)].astype(f32)
            for u in range(unroll):
                to = (i * unroll + u) * PITCH
                plain[pl.ds(to, STA), :] = x[:, u * LANES : (u + 1) * LANES]
            return carry

        for h in range(2):
            copies[p * 2 + h].wait()
            lax.fori_loop(h * steps // 2, (h + 1) * steps // 2, fill, 0, unroll=4)
        lax.fori_loop(0, FRONT // unroll, wrap, 0, unroll=2)
    for q in range(0, STA, 2):
        for p in range(2):
            x = []
            for i in range(2):
                coarse = lax.shift_right_logical(delay_ref[q + i], 7)
                first = (FRONT - 8 - coarse) * PITCH + q + i
                x.append(plain_ref.at[p][pl.ds(first, rows, stride=PITCH), :].astype(bf16))
            y = jnp.dot(jnp.concatenate(x, axis=1), matrices[q // 2], preferred_element_type=f32)
            for i in range(2):
                turned_ref.at[p][pl.ds(q + i, rows, stride=PITCH), :] = y[:, i * LANES : (i + 1) * LANES]

    for out_ref, hop in zip(out_refs, HOPS):
        first = neighbour(hop, 1) * TILES

        def merge(i, before):
            at = pl.multiple_of(i * (unroll * LANES), unroll * LANES)
            last = []
            for p in range(2):
                parts = []
                old = before[p]
                for u in range(unroll):
                    tile = 8 + first + i * unroll + u
                    now = turned_ref[p, pl.ds(tile * PITCH, STA), :]
                    parts.append(jnp.where(keep, now, old))
                    old = now
                out_ref[p, :, pl.ds(at, unroll * LANES)] = jnp.concatenate(parts, axis=1).astype(bf16)
                last.append(old)
            return tuple(last)

        start = tuple(turned_ref[p, pl.ds((7 + first) * PITCH, STA), :] for p in range(2))
        lax.fori_loop(0, TILES // unroll, merge, start, unroll=4)


def beam_kernel(w_ref, after_ref, *refs):
    v_refs, out_refs, sums_ref = refs[:STA], refs[STA : 2 * STA], refs[2 * STA]
    w = w_ref[0].astype(f32)
    rows = []
    for d in range(STA):
        w_re = w[0, d * BEAMS : (d + 1) * BEAMS]
        w_im = w[1, d * BEAMS : (d + 1) * BEAMS]
        rows.append(jnp.concatenate([w_re, -w_im], axis=1))
        rows.append(jnp.concatenate([w_im, w_re], axis=1))
    left = jnp.concatenate(rows, axis=0).astype(bf16)
    old = lax.broadcasted_iota(jnp.int32, (128, 128), 0)
    new = lax.broadcasted_iota(jnp.int32, (128, 128), 1)
    group = lax.shift_right_logical(new, 3) & 7
    wanted = (new & 64) | (new & 7)
    for r, hop in enumerate(HOPS):
        wanted = jnp.where(group == r, wanted + neighbour(hop, -1) * 8, wanted)
    left = jnp.dot(left, (old == wanted).astype(f32).astype(bf16), preferred_element_type=f32).astype(bf16)
    new = lax.broadcasted_iota(jnp.int32, (64, 64), 0)
    old = lax.broadcasted_iota(jnp.int32, (64, 64), 1)
    group = lax.shift_right_logical(new, 3)
    wanted = new & 7
    for r, hop in enumerate(HOPS):
        wanted = jnp.where(group == r, wanted + neighbour(hop, 1) * 8, wanted)
    left = jnp.dot((old == wanted).astype(f32).astype(bf16), left, preferred_element_type=f32).astype(bf16)
    chunk = 1024
    peak = jnp.zeros((64, LANES), f32)
    for i in range(BLOCK // chunk):
        at = slice(i * chunk, (i + 1) * chunk)
        volts = jnp.concatenate([v[0, :, at] for v in v_refs] + [v[1, :, at] for v in v_refs], axis=0)
        sums = jnp.dot(left, volts, preferred_element_type=f32)
        sums_ref[:, at] = sums
        for u in range(chunk // LANES):
            peak = jnp.maximum(peak, jnp.abs(sums[:, u * LANES : (u + 1) * LANES]))
    code = code_of(peak)
    inverse = LEVELS / scale_of(code)
    for d in range(STA):
        at8 = slice(d * 8, d * 8 + 8)
        factor = inverse[at8]
        out_ref = out_refs[d]
        out_ref[:, BLOCK:] = code[at8].astype(jnp.int32).astype(jnp.int16)

        def pack(i, carry):
            at = pl.multiple_of(i * 1024, 1024)
            x = sums_ref[at8, pl.ds(at, 1024)]
            x = x * jnp.concatenate([factor] * 8, axis=1)
            out_ref[:, pl.ds(at, 1024)] = jnp.round(x).astype(jnp.int32).astype(jnp.int16)
            return carry

        lax.fori_loop(0, BLOCK // 1024, pack, 0, unroll=4)


def halves(x, axis):
    high = x.astype(bf16)
    low = (x - high.astype(f32)).astype(bf16)
    return jnp.concatenate([high, low, high], axis=axis)


def dot_left(table_ref, parity, u):
    high, low = table_ref[parity, 0], table_ref[parity, 1]
    return jnp.dot(jnp.concatenate([high, high, low], axis=1), halves(u, 0), preferred_element_type=f32)


def dot_right(u, table_ref, parity):
    high, low = table_ref[parity, 0], table_ref[parity, 1]
    return jnp.dot(halves(u, 1), jnp.concatenate([high, high, low], axis=0), preferred_element_type=f32)


QUARTER_HIGH = 1.5703125
QUARTER_LOW = float(np.float32(np.pi / 2 - QUARTER_HIGH))


def cos_sin(phase):
    turns = jnp.round(phase * (2 / np.pi))
    r = (phase - turns * QUARTER_HIGH) - turns * QUARTER_LOW
    quadrant = turns.astype(jnp.int32)
    z = r * r
    s = r + r * z * (-1.6666654611e-1 + z * (8.3321608736e-3 + z * (-1.9515295891e-4)))
    c = 1.0 - 0.5 * z + z * z * (4.166664568298827e-2 + z * (-1.388731625493765e-3 + z * 2.443315711809948e-5))
    odd = (quadrant & 1) == 1
    cos = jnp.where(odd, s, c)
    sin = jnp.where(odd, c, s)
    cos = jnp.where(((quadrant + 1) & 2) == 2, -cos, cos)
    sin = jnp.where((quadrant & 2) == 2, -sin, sin)
    return cos, sin


def chirp_kernel(dm_ref, after_ref, out_ref):
    centre = BASE_FREQ + CHANNEL_WIDTH * (lax.axis_index("sub").astype(f32) + 0.5)
    row = lax.broadcasted_iota(jnp.int32, (8, ROOT), 0)
    col = lax.broadcasted_iota(jnp.int32, (8, ROOT), 1)
    k2 = ROOT * (2 * (col & (HALF - 1)) + lax.shift_right_logical(col, 7))
    measures = [DM_STEP * dm_ref[b].astype(f32) for b in range(BEAMS)]

    def chirp(i, carry):
        at = pl.ds(pl.multiple_of(i * 8, 8), 8)
        k1 = 2 * ((row + i * 8) & (HALF - 1)) + i // (HALF // 8)
        position = k1 + k2
        signed = jnp.where(position < TOTAL // 2, position, position - TOTAL)
        offset = CHANNEL_WIDTH * signed.astype(f32) / TOTAL
        base = (TWO_PI * DISPERSION) * offset * offset / (centre * centre * (centre + offset))
        for b in range(BEAMS):
            c, s = cos_sin(measures[b] * base)
            out_ref[b, 0, at, :] = c
            out_ref[b, 1, at, :] = s
        return carry

    lax.fori_loop(0, ROOT // 8, chirp, 0, unroll=2)


def dedisperse_kernel(
    chirp_ref, fwd_ref, bwd_ref, end_ref, tw_ref, *refs
):
    x_refs, out_ref, time_ref, last_ref = refs[:STA], refs[STA], refs[STA + 1], refs[STA + 2]
    for x_ref, hop in zip(x_refs, HOPS):
        scale = scale_of(widen(x_ref[:, BLOCK:])) * (1.0 / LEVELS)
        first_tile = neighbour(hop, -1) * TILES

        def decode(i, carry):
            at = pl.multiple_of(i * 512, 512)
            x = widen(x_ref[:, pl.ds(at, 512)])
            for u in range(4):
                time_ref[pl.ds((first_tile + i * 4 + u) * PITCH, 8), :] = x[:, u * LANES : (u + 1) * LANES] * scale
            return carry

        lax.fori_loop(0, TILES // 4, decode, 0, unroll=4)

    def beam(b):
        x = []
        for p in range(2):
            x.append(
                jnp.concatenate([time_ref[pl.ds(h * PITCH + p * 4 + b, ROOT, stride=2 * PITCH), :] for h in range(2)], axis=1)
            )
        yield
        outs = []
        for parity in range(2):
            u = [v[:HALF] + v[HALF:] if parity == 0 else v[:HALF] - v[HALF:] for v in x]
            u = jnp.concatenate(u, axis=0)
            outs.append(dot_left(fwd_ref, parity, u))
        yield
        re = jnp.concatenate([o[:HALF] for o in outs], axis=0)
        im = jnp.concatenate([o[HALF:] for o in outs], axis=0)
        tw_re, tw_im = tw_ref[0], tw_ref[1]
        re, im = re * tw_re + im * tw_im, im * tw_re - re * tw_im
        outs = []
        for parity in range(2):
            u = [v[:, :HALF] + v[:, HALF:] if parity == 0 else v[:, :HALF] - v[:, HALF:] for v in (re, im)]
            u = jnp.concatenate(u, axis=1)
            outs.append(dot_right(u, bwd_ref, parity))
        yield
        sums = []
        for parity in range(2):
            at = slice(parity * HALF, (parity + 1) * HALF)
            c, s = chirp_ref[b, 0, :, at], chirp_ref[b, 1, :, at]
            y_re, y_im = outs[parity][:, :HALF], outs[parity][:, HALF:]
            u = jnp.concatenate([y_re * c - y_im * s, y_re * s + y_im * c], axis=1)
            sums.append(dot_right(u, fwd_ref, parity))
        yield
        top, bottom = sums[0] + sums[1], sums[0] - sums[1]
        re = jnp.concatenate([top[:, :HALF], bottom[:, :HALF]], axis=1)
        im = jnp.concatenate([top[:, HALF:], bottom[:, HALF:]], axis=1)
        re, im = re * tw_re - im * tw_im, im * tw_re + re * tw_im
        sums = []
        for parity in range(2):
            at = slice(parity * HALF, (parity + 1) * HALF)
            u = jnp.concatenate([re[at], im[at]], axis=0)
            sums.append(dot_left(end_ref, parity, u))
        yield
        top, bottom = sums[0] + sums[1], sums[0] - sums[1]
        for p in range(2):
            for r in range(2):
                at = slice(p * HALF + r * 64, p * HALF + r * 64 + 64)
                for h in range(2):
                    lanes = slice(h * LANES, (h + 1) * LANES)
                    first = b * 4 + r * 2 + h
                    last_ref[p, first, :64] = top[at, lanes]
                    last_ref[p, first, 64:] = bottom[at, lanes]

    running = [beam(b) for b in range(BEAMS)]
    for tick in range(1 * (BEAMS - 1) + 6):
        for b in range(BEAMS):
            if tick >= 1 * b:
                next(running[b], None)

    def encode(i, carry):
        at = pl.ds(pl.multiple_of(i * 8, 8), 8)
        x = [[last_ref[p, k, at, :] for k in range(16)] for p in range(2)]
        peak = jnp.abs(x[0][0])
        for k in range(1, 32):
            peak = jnp.maximum(peak, jnp.abs(x[k // 16][k % 16]))
        code = code_of(peak)
        inverse = LEVELS / scale_of(code)
        first = i * (8 * ROWS)
        for k in range(16):
            low = jnp.round(x[0][k] * inverse).astype(jnp.int32) & 0xFFFF
            high = jnp.round(x[1][k] * inverse).astype(jnp.int32) << 16
            out_ref[pl.ds(first + k, 8, stride=ROWS), :] = low | high
        out_ref[pl.ds(first + 16, 8, stride=ROWS), :] = code.astype(jnp.int32)
        return carry

    lax.fori_loop(0, DEVICES // 8, encode, 0, unroll=2)


def finish_kernel(x_ref, out_hbm, power_ref, out_ref, sems):
    copies = []
    for sub in range(16):
        code = x_ref[pl.ds(sub * STA * ROWS + 16, STA, stride=ROWS), :]
        scales = scale_of(code.astype(f32)) * (1.0 / LEVELS)
        for sta in range(STA):
            src = (sub * STA + sta) * ROWS
            to = sub * 256 + sta * 16
            scale = jnp.broadcast_to(scales[sta : sta + 1], (16, LANES))
            both = x_ref[src : src + 16, :]
            out_ref[to : to + 16, :] = ((both << 16) >> 16).astype(f32) * scale
            out_ref[to + 128 : to + 144, :] = (both >> 16).astype(f32) * scale
        rows = pl.ds(sub * 256, 256)
        copies.append(pltpu.make_async_copy(out_ref.at[rows], out_hbm.at[rows], sems.at[sub]))
        copies[-1].start()
    for i in range(16):
        power = jnp.zeros((8, LANES), f32)
        for sub in range(16):
            re = out_ref[sub * 256 + i * 8 : sub * 256 + i * 8 + 8, :]
            im = out_ref[sub * 256 + 128 + i * 8 : sub * 256 + 136 + i * 8, :]
            power = power + (re * re + im * im)
        power_ref[i * 8 : i * 8 + 8, :] = power * (1.0 / 16.0)
    for copy in copies:
        copy.wait()


VMEM = pl.BlockSpec(memory_space=pltpu.VMEM)
SMEM = pl.BlockSpec(memory_space=pltpu.SMEM)
HBM = pl.BlockSpec(memory_space=pltpu.HBM)
PARAMS = pltpu.CompilerParams(vmem_limit_bytes=36 * 1024 * 1024)


SHIFT_PARAMS = pltpu.CompilerParams(vmem_limit_bytes=50 * 1024 * 1024 + 512 * 1024)


def shift(voltages, delays):
    return pl.pallas_call(
        shift_kernel,
        out_shape=[jax.ShapeDtypeStruct((2, STA, BLOCK), bf16)] * STA,
        in_specs=[HBM, HBM],
        out_specs=[VMEM] * STA,
        scratch_shapes=[
            pltpu.VMEM((2, STA, TOTAL), bf16),
            pltpu.SMEM((STA,), jnp.int32),
            pltpu.VMEM((2, (TOTAL // LANES + FRONT) * PITCH, LANES), f32),
            pltpu.VMEM((2, (TOTAL // LANES + 8) * PITCH, LANES), f32),
            pltpu.SemaphoreType.DMA((5,)),
        ],
        compiler_params=SHIFT_PARAMS,
        name="shift",
    )(delays, voltages)


def beamform(volts, weights, after):
    return pl.pallas_call(
        beam_kernel,
        out_shape=[jax.ShapeDtypeStruct((8, BLOCK + LANES), jnp.int16)] * STA,
        in_specs=[VMEM, HBM] + [VMEM] * STA,
        out_specs=[VMEM] * STA,
        scratch_shapes=[pltpu.VMEM((64, BLOCK), f32)],
        compiler_params=PARAMS,
        name="beamform",
    )(weights, after, *volts)


def chirps(dm_index, after):
    return pl.pallas_call(
        chirp_kernel,
        out_shape=jax.ShapeDtypeStruct((BEAMS, 2, ROOT, ROOT), f32),
        in_specs=[SMEM, HBM],
        out_specs=VMEM,
        compiler_params=PARAMS,
        cost_estimate=pl.CostEstimate(flops=20_000_000, transcendentals=0, bytes_accessed=2 << 20),
        name="chirps",
    )(dm_index, after)


def dedisperse(chirp, coded):
    fwd, bwd, end, tw = tables()
    return pl.pallas_call(
        dedisperse_kernel,
        out_shape=jax.ShapeDtypeStruct((DEVICES * ROWS, LANES), jnp.int32),
        in_specs=[VMEM] * (5 + STA),
        out_specs=VMEM,
        scratch_shapes=[
            pltpu.VMEM((TOTAL // LANES * PITCH, LANES), f32),
            pltpu.VMEM((2, 16, DEVICES, LANES), f32),
        ],
        compiler_params=PARAMS,
        name="dedisperse",
    )(chirp, fwd, bwd, end, tw, *coded)


def finish(coded):
    return pl.pallas_call(
        finish_kernel,
        out_shape=(jax.ShapeDtypeStruct((4096, LANES), f32), jax.ShapeDtypeStruct((128, LANES), f32)),
        in_specs=[VMEM],
        out_specs=(HBM, VMEM),
        scratch_shapes=[pltpu.VMEM((4096, LANES), f32), pltpu.SemaphoreType.DMA((16,))],
        compiler_params=PARAMS,
        name="finish",
    )(coded)


def exchange(blocks):
    received = [blocks[0]]
    for block, hop in zip(blocks[1:], HOPS[1:]):
        pairs = [(x * 4 + y, (x + hop[0]) % 2 * 4 + (y + hop[1]) % 4) for x in range(2) for y in range(4)]
        received.append(lax.ppermute(block, "sta", pairs))
    return received


def shards(voltages, beam_weights, station_delays, dm_index):
    blocks = shift(voltages, station_delays)
    chirp = chirps(dm_index.reshape(BEAMS), blocks[0])
    coded = exchange(beamform(exchange(blocks), beam_weights, chirp))
    coded = dedisperse(chirp, coded).reshape(DEVICES, 1, ROWS * LANES)
    coded = lax.all_to_all(coded, ("sub", "sta"), 0, 0, tiled=True).reshape(DEVICES * ROWS, LANES)
    moved, intensity = finish(coded)
    return moved.reshape(16, 2, 32, 1, 512), intensity.reshape(32, 1, 512)


def solution(mesh):
    return jax.shard_map(
        shards,
        mesh=mesh,
        in_specs=(
            P("sub", None, "sta", None),
            P("sub", None, None, None),
            P("sta"),
            P("sta", None),
        ),
        out_specs=(P(None, None, None, None, ("sub", "sta")), P(None, None, ("sub", "sta"))),
        check_vma=False,
    )
```

```python
import functools

import jax
import jax.numpy as jnp
import numpy as np
from jax import lax
from jax.experimental import pallas as pl
from jax.experimental.pallas import tpu as pltpu
from jax.sharding import PartitionSpec as P

TWO_PI = 6.283185307179586
DISPERSION = 4148808000.0
DM_STEP = 10.0
BASE_FREQ = 120.0
CHANNEL_WIDTH = 0.1953125

TOTAL = 65536
ROOT = 256
HALF = 128
LANES = 128
STA = 8
BLOCK = TOTAL // STA
TILES = BLOCK // LANES
BEAMS = 4
DEVICES = 128
ROWS = 17
CODE_STEP = 64.0
LEVELS = 32767.0
FLOOR = 1e-33

HOPS = [(0, 0), (1, 0), (0, 2), (1, 2), (0, 1), (1, 1), (0, 3), (1, 3)]


f32 = jnp.float32
bf16 = jnp.bfloat16


def neighbour(hop, sign):
    me = lax.axis_index("sta")
    x = (lax.shift_right_logical(me, 2) + hop[0]) & 1
    y = ((me & 3) + sign * hop[1]) & 3
    return x * 4 + y


def split_np(table):
    high = table.astype(bf16)
    low = (table - high.astype(np.float64)).astype(bf16)
    return high, low


@functools.lru_cache(maxsize=None)
def tables():
    m = np.arange(HALF)
    fwd = []
    for parity in range(2):
        angle = 2 * np.pi * (((2 * m[:, None] + parity) * m[None, :]) % ROOT) / ROOT
        c, s = np.cos(angle), np.sin(angle)
        fwd.append(np.block([[c, s], [-s, c]]))
    fwd = np.stack(fwd)
    bwd = fwd.transpose(0, 2, 1)
    order = (2 * np.arange(64)[None, :] + np.arange(2)[:, None]).reshape(-1)
    order = np.concatenate([order, HALF + order])
    last = bwd[:, order, :] / TOTAL

    def pair(t):
        return np.stack(split_np(t), axis=1)

    rows = np.concatenate([2 * m, 2 * m + 1])
    angle = 2 * np.pi * (rows[:, None] * np.arange(ROOT)[None, :]) / TOTAL
    twiddle = np.stack([np.cos(angle), np.sin(angle)]).astype(np.float32)
    return pair(fwd), pair(bwd), pair(last), twiddle


def code_of(peak):
    return jnp.ceil(jnp.log(jnp.maximum(peak, FLOOR)) * (CODE_STEP / 0.6931471805599453)) + 1.0


def scale_of(code):
    return jnp.exp2(code * (1.0 / CODE_STEP))


def quantize(x, inverse):
    return jnp.round(x * inverse).astype(jnp.int32).astype(jnp.int16)


def widen(q):
    return q.astype(jnp.int32).astype(f32)


PITCH = 9
FRONT = 136


def shift_kernel(delay_hbm, v_hbm, *refs):
    out_refs = refs[:STA]
    v_ref, delay_ref, plain_ref, turned_ref, sems = refs[STA:]
    halves_at = [pl.ds(h * (TOTAL // 2), TOTAL // 2) for h in range(2)]
    delays = pltpu.make_async_copy(delay_hbm, delay_ref, sems.at[4])
    delays.start()
    copies = []
    for p in range(2):
        for h in range(2):
            source, to = v_hbm.at[0, p, :, halves_at[h]], v_ref.at[p, :, halves_at[h]]
            copies.append(pltpu.make_async_copy(source, to, sems.at[p * 2 + h]))
            copies[-1].start()
    delays.wait()
    count = TOTAL // LANES
    lane = lax.broadcasted_iota(jnp.int32, (STA, LANES), 1)
    row = lax.broadcasted_iota(jnp.int32, (STA, LANES), 0)
    fine = jnp.zeros((STA, LANES), jnp.int32)
    for q in range(STA):
        fine = jnp.where(row == q, delay_ref[q] & (LANES - 1), fine)
    keep = lane >= fine
    source = lax.broadcasted_iota(jnp.int32, (LANES, LANES), 0)
    target = lax.broadcasted_iota(jnp.int32, (LANES, LANES), 1)
    turn = (target - source) & (LANES - 1)
    none = jnp.zeros((LANES, LANES), bf16)
    matrices = []
    for q in range(0, STA, 2):
        pair = [(turn == (delay_ref[q + i] & (LANES - 1))).astype(f32).astype(bf16) for i in range(2)]
        top = jnp.concatenate([pair[0], none], axis=1)
        low = jnp.concatenate([none, pair[1]], axis=1)
        matrices.append(jnp.concatenate([top, low], axis=0))
    unroll = 8
    rows = count + 8
    steps = count // unroll
    for p in range(2):
        plain = plain_ref.at[p]

        def fill(i, carry):
            at = pl.multiple_of(i * (unroll * LANES), unroll * LANES)
            x = v_ref[p, :, pl.ds(at, unroll * LANES)].astype(f32)
            for u in range(unroll):
                to = (FRONT + i * unroll + u) * PITCH
                plain[pl.ds(to, STA), :] = x[:, u * LANES : (u + 1) * LANES]
            return carry

        def wrap(i, carry):
            at = pl.multiple_of((TOTAL - FRONT * LANES) + i * (unroll * LANES), unroll * LANES)
            x = v_ref[p, :, pl.ds(at, unroll * LANES)].astype(f32)
            for u in range(unroll):
                to = (i * unroll + u) * PITCH
                plain[pl.ds(to, STA), :] = x[:, u * LANES : (u + 1) * LANES]
            return carry

        for h in range(2):
            copies[p * 2 + h].wait()
            lax.fori_loop(h * steps // 2, (h + 1) * steps // 2, fill, 0, unroll=4)
        lax.fori_loop(0, FRONT // unroll, wrap, 0, unroll=2)
    for q in range(0, STA, 2):
        for p in range(2):
            x = []
            for i in range(2):
                coarse = lax.shift_right_logical(delay_ref[q + i], 7)
                first = (FRONT - 8 - coarse) * PITCH + q + i
                x.append(plain_ref.at[p][pl.ds(first, rows, stride=PITCH), :].astype(bf16))
            y = jnp.dot(jnp.concatenate(x, axis=1), matrices[q // 2], preferred_element_type=f32)
            for i in range(2):
                turned_ref.at[p][pl.ds(q + i, rows, stride=PITCH), :] = y[:, i * LANES : (i + 1) * LANES]

    for out_ref, hop in zip(out_refs, HOPS):
        first = neighbour(hop, 1) * TILES

        def merge(i, before):
            at = pl.multiple_of(i * (unroll * LANES), unroll * LANES)
            last = []
            for p in range(2):
                parts = []
                old = before[p]
                for u in range(unroll):
                    tile = 8 + first + i * unroll + u
                    now = turned_ref[p, pl.ds(tile * PITCH, STA), :]
                    parts.append(jnp.where(keep, now, old))
                    old = now
                out_ref[p, :, pl.ds(at, unroll * LANES)] = jnp.concatenate(parts, axis=1).astype(bf16)
                last.append(old)
            return tuple(last)

        start = tuple(turned_ref[p, pl.ds((7 + first) * PITCH, STA), :] for p in range(2))
        lax.fori_loop(0, TILES // unroll, merge, start, unroll=4)


def beam_kernel(left_ref, *refs):
    v_refs, out_refs, sums_ref = refs[:STA], refs[STA : 2 * STA], refs[2 * STA]
    left = left_ref[...]
    chunk = 1024
    peak = jnp.zeros((64, LANES), f32)
    for i in range(BLOCK // chunk):
        at = slice(i * chunk, (i + 1) * chunk)
        volts = jnp.concatenate([v[0, :, at] for v in v_refs] + [v[1, :, at] for v in v_refs], axis=0)
        sums = jnp.dot(left, volts, preferred_element_type=f32)
        sums_ref[:, at] = sums
        for u in range(chunk // LANES):
            peak = jnp.maximum(peak, jnp.abs(sums[:, u * LANES : (u + 1) * LANES]))
    code = code_of(peak)
    inverse = LEVELS / scale_of(code)
    for d in range(STA):
        at8 = slice(d * 8, d * 8 + 8)
        factor = inverse[at8]
        out_ref = out_refs[d]
        out_ref[:, BLOCK:] = code[at8].astype(jnp.int32).astype(jnp.int16)

        def pack(i, carry):
            at = pl.multiple_of(i * 1024, 1024)
            x = sums_ref[at8, pl.ds(at, 1024)]
            x = x * jnp.concatenate([factor] * 8, axis=1)
            out_ref[:, pl.ds(at, 1024)] = jnp.round(x).astype(jnp.int32).astype(jnp.int16)
            return carry

        lax.fori_loop(0, BLOCK // 1024, pack, 0, unroll=4)


def halves(x, axis):
    high = x.astype(bf16)
    low = (x - high.astype(f32)).astype(bf16)
    return jnp.concatenate([high, low, high], axis=axis)


def dot_left(table_ref, parity, u):
    high, low = table_ref[parity, 0], table_ref[parity, 1]
    return jnp.dot(jnp.concatenate([high, high, low], axis=1), halves(u, 0), preferred_element_type=f32)


def dot_right(u, table_ref, parity):
    high, low = table_ref[parity, 0], table_ref[parity, 1]
    return jnp.dot(halves(u, 1), jnp.concatenate([high, high, low], axis=0), preferred_element_type=f32)


QUARTER_HIGH = 1.5703125
QUARTER_LOW = float(np.float32(np.pi / 2 - QUARTER_HIGH))


def cos_sin(phase):
    turns = jnp.round(phase * (2 / np.pi))
    r = (phase - turns * QUARTER_HIGH) - turns * QUARTER_LOW
    quadrant = turns.astype(jnp.int32)
    z = r * r
    s = r + r * z * (-1.6666654611e-1 + z * (8.3321608736e-3 + z * (-1.9515295891e-4)))
    c = 1.0 - 0.5 * z + z * z * (4.166664568298827e-2 + z * (-1.388731625493765e-3 + z * 2.443315711809948e-5))
    odd = (quadrant & 1) == 1
    cos = jnp.where(odd, s, c)
    sin = jnp.where(odd, c, s)
    cos = jnp.where(((quadrant + 1) & 2) == 2, -cos, cos)
    sin = jnp.where((quadrant & 2) == 2, -sin, sin)
    return cos, sin


def tables_kernel(dm_ref, after_ref, w_ref, out_ref, left_ref):
    w = w_ref[0].astype(f32)
    rows = []
    for d in range(STA):
        w_re = w[0, d * BEAMS : (d + 1) * BEAMS]
        w_im = w[1, d * BEAMS : (d + 1) * BEAMS]
        rows.append(jnp.concatenate([w_re, -w_im], axis=1))
        rows.append(jnp.concatenate([w_im, w_re], axis=1))
    left = jnp.concatenate(rows, axis=0).astype(bf16)
    old = lax.broadcasted_iota(jnp.int32, (128, 128), 0)
    new = lax.broadcasted_iota(jnp.int32, (128, 128), 1)
    group = lax.shift_right_logical(new, 3) & 7
    wanted = (new & 64) | (new & 7)
    for r, hop in enumerate(HOPS):
        wanted = jnp.where(group == r, wanted + neighbour(hop, -1) * 8, wanted)
    left = jnp.dot(left, (old == wanted).astype(f32).astype(bf16), preferred_element_type=f32).astype(bf16)
    new = lax.broadcasted_iota(jnp.int32, (64, 64), 0)
    old = lax.broadcasted_iota(jnp.int32, (64, 64), 1)
    group = lax.shift_right_logical(new, 3)
    wanted = new & 7
    for r, hop in enumerate(HOPS):
        wanted = jnp.where(group == r, wanted + neighbour(hop, 1) * 8, wanted)
    left = jnp.dot((old == wanted).astype(f32).astype(bf16), left, preferred_element_type=f32).astype(bf16)
    left_ref[...] = left
    centre = BASE_FREQ + CHANNEL_WIDTH * (lax.axis_index("sub").astype(f32) + 0.5)
    row = lax.broadcasted_iota(jnp.int32, (8, ROOT), 0)
    col = lax.broadcasted_iota(jnp.int32, (8, ROOT), 1)
    k2 = ROOT * (2 * (col & (HALF - 1)) + lax.shift_right_logical(col, 7))
    measures = [DM_STEP * dm_ref[b].astype(f32) for b in range(BEAMS)]

    def chirp(i, carry):
        at = pl.ds(pl.multiple_of(i * 8, 8), 8)
        k1 = 2 * ((row + i * 8) & (HALF - 1)) + i // (HALF // 8)
        position = k1 + k2
        signed = jnp.where(position < TOTAL // 2, position, position - TOTAL)
        offset = CHANNEL_WIDTH * signed.astype(f32) / TOTAL
        base = (TWO_PI * DISPERSION) * offset * offset / (centre * centre * (centre + offset))
        for b in range(BEAMS):
            c, s = cos_sin(measures[b] * base)
            out_ref[b, 0, at, :] = c
            out_ref[b, 1, at, :] = s
        return carry

    lax.fori_loop(0, ROOT // 8, chirp, 0, unroll=2)


def dedisperse_kernel(
    chirp_ref, fwd_ref, bwd_ref, end_ref, tw_ref, *refs
):
    x_refs, out_ref, time_ref, last_ref = refs[:STA], refs[STA], refs[STA + 1], refs[STA + 2]
    for x_ref, hop in zip(x_refs, HOPS):
        scale = scale_of(widen(x_ref[:, BLOCK:])) * (1.0 / LEVELS)
        first_tile = neighbour(hop, -1) * TILES

        def decode(i, carry):
            at = pl.multiple_of(i * 512, 512)
            x = widen(x_ref[:, pl.ds(at, 512)])
            for u in range(4):
                time_ref[pl.ds((first_tile + i * 4 + u) * PITCH, 8), :] = x[:, u * LANES : (u + 1) * LANES] * scale
            return carry

        lax.fori_loop(0, TILES // 4, decode, 0, unroll=4)

    def beam(b):
        x = []
        for p in range(2):
            x.append(
                jnp.concatenate([time_ref[pl.ds(h * PITCH + p * 4 + b, ROOT, stride=2 * PITCH), :] for h in range(2)], axis=1)
            )
        yield
        outs = []
        for parity in range(2):
            u = [v[:HALF] + v[HALF:] if parity == 0 else v[:HALF] - v[HALF:] for v in x]
            u = jnp.concatenate(u, axis=0)
            outs.append(dot_left(fwd_ref, parity, u))
        yield
        re = jnp.concatenate([o[:HALF] for o in outs], axis=0)
        im = jnp.concatenate([o[HALF:] for o in outs], axis=0)
        tw_re, tw_im = tw_ref[0], tw_ref[1]
        re, im = re * tw_re + im * tw_im, im * tw_re - re * tw_im
        outs = []
        for parity in range(2):
            u = [v[:, :HALF] + v[:, HALF:] if parity == 0 else v[:, :HALF] - v[:, HALF:] for v in (re, im)]
            u = jnp.concatenate(u, axis=1)
            outs.append(dot_right(u, bwd_ref, parity))
        yield
        sums = []
        for parity in range(2):
            at = slice(parity * HALF, (parity + 1) * HALF)
            c, s = chirp_ref[b, 0, :, at], chirp_ref[b, 1, :, at]
            y_re, y_im = outs[parity][:, :HALF], outs[parity][:, HALF:]
            u = jnp.concatenate([y_re * c - y_im * s, y_re * s + y_im * c], axis=1)
            sums.append(dot_right(u, fwd_ref, parity))
        yield
        top, bottom = sums[0] + sums[1], sums[0] - sums[1]
        re = jnp.concatenate([top[:, :HALF], bottom[:, :HALF]], axis=1)
        im = jnp.concatenate([top[:, HALF:], bottom[:, HALF:]], axis=1)
        re, im = re * tw_re - im * tw_im, im * tw_re + re * tw_im
        sums = []
        for parity in range(2):
            at = slice(parity * HALF, (parity + 1) * HALF)
            u = jnp.concatenate([re[at], im[at]], axis=0)
            sums.append(dot_left(end_ref, parity, u))
        yield
        top, bottom = sums[0] + sums[1], sums[0] - sums[1]
        for p in range(2):
            for r in range(2):
                at = slice(p * HALF + r * 64, p * HALF + r * 64 + 64)
                for h in range(2):
                    lanes = slice(h * LANES, (h + 1) * LANES)
                    first = b * 4 + r * 2 + h
                    last_ref[p, first, :64] = top[at, lanes]
                    last_ref[p, first, 64:] = bottom[at, lanes]

    running = [beam(b) for b in range(BEAMS)]
    for tick in range(6):
        for b in range(BEAMS):
            if tick >= 0 * b:
                next(running[b], None)

    def encode(i, carry):
        at = pl.ds(pl.multiple_of(i * 8, 8), 8)
        x = [[last_ref[p, k, at, :] for k in range(16)] for p in range(2)]
        peak = jnp.abs(x[0][0])
        for k in range(1, 32):
            peak = jnp.maximum(peak, jnp.abs(x[k // 16][k % 16]))
        code = code_of(peak)
        inverse = LEVELS / scale_of(code)
        first = i * (8 * ROWS)
        for k in range(16):
            low = jnp.round(x[0][k] * inverse).astype(jnp.int32) & 0xFFFF
            high = jnp.round(x[1][k] * inverse).astype(jnp.int32) << 16
            out_ref[pl.ds(first + k, 8, stride=ROWS), :] = low | high
        out_ref[pl.ds(first + 16, 8, stride=ROWS), :] = code.astype(jnp.int32)
        return carry

    lax.fori_loop(0, DEVICES // 8, encode, 0, unroll=4)


SUBS = 4


def finish_kernel(x_ref, out_ref, power_ref):
    step = pl.program_id(0)

    @pl.when(step == 0)
    def _():
        power_ref[...] = jnp.zeros_like(power_ref)

    scales = []
    for sub in range(SUBS):
        code = x_ref[pl.ds(sub * STA * ROWS + 16, STA, stride=ROWS), :]
        scales.append(scale_of(code.astype(f32)) * (1.0 / LEVELS))
    for sta in range(STA):
        power = power_ref[sta * 16 : sta * 16 + 16, :]
        for sub in range(SUBS):
            src = (sub * STA + sta) * ROWS
            to = sub * 256 + sta * 16
            scale = jnp.broadcast_to(scales[sub][sta : sta + 1], (16, LANES))
            both = x_ref[src : src + 16, :]
            re = ((both << 16) >> 16).astype(f32) * scale
            im = (both >> 16).astype(f32) * scale
            out_ref[to : to + 16, :] = re
            out_ref[to + 128 : to + 144, :] = im
            power = power + (re * re + im * im)
        power_ref[sta * 16 : sta * 16 + 16, :] = power

    @pl.when(step == pl.num_programs(0) - 1)
    def _():
        power_ref[...] = power_ref[...] * (1.0 / 16.0)


VMEM = pl.BlockSpec(memory_space=pltpu.VMEM)
SMEM = pl.BlockSpec(memory_space=pltpu.SMEM)
HBM = pl.BlockSpec(memory_space=pltpu.HBM)
PARAMS = pltpu.CompilerParams(vmem_limit_bytes=36 * 1024 * 1024)


SHIFT_PARAMS = pltpu.CompilerParams(vmem_limit_bytes=50 * 1024 * 1024 + 512 * 1024)


def shift(voltages, delays):
    return pl.pallas_call(
        shift_kernel,
        out_shape=[jax.ShapeDtypeStruct((2, STA, BLOCK), bf16)] * STA,
        in_specs=[HBM, HBM],
        out_specs=[VMEM] * STA,
        scratch_shapes=[
            pltpu.VMEM((2, STA, TOTAL), bf16),
            pltpu.SMEM((STA,), jnp.int32),
            pltpu.VMEM((2, (TOTAL // LANES + FRONT) * PITCH, LANES), f32),
            pltpu.VMEM((2, (TOTAL // LANES + 8) * PITCH, LANES), f32),
            pltpu.SemaphoreType.DMA((5,)),
        ],
        compiler_params=SHIFT_PARAMS,
        name="shift",
    )(delays, voltages)


def beamform(volts, left):
    return pl.pallas_call(
        beam_kernel,
        out_shape=[jax.ShapeDtypeStruct((8, BLOCK + LANES), jnp.int16)] * STA,
        in_specs=[VMEM] * (1 + STA),
        out_specs=[VMEM] * STA,
        scratch_shapes=[pltpu.VMEM((64, BLOCK), f32)],
        compiler_params=PARAMS,
        name="beamform",
    )(left, *volts)


def chirps(dm_index, after, weights):
    return pl.pallas_call(
        tables_kernel,
        out_shape=(
            jax.ShapeDtypeStruct((BEAMS, 2, ROOT, ROOT), f32),
            jax.ShapeDtypeStruct((64, 128), bf16),
        ),
        in_specs=[SMEM, HBM, VMEM],
        out_specs=(VMEM, VMEM),
        compiler_params=PARAMS,
        cost_estimate=pl.CostEstimate(flops=20_000_000, transcendentals=0, bytes_accessed=2 << 20),
        name="chirps",
    )(dm_index, after, weights)


def dedisperse(chirp, coded):
    fwd, bwd, end, tw = tables()
    return pl.pallas_call(
        dedisperse_kernel,
        out_shape=jax.ShapeDtypeStruct((DEVICES * ROWS, LANES), jnp.int32),
        in_specs=[VMEM] * (5 + STA),
        out_specs=VMEM,
        scratch_shapes=[
            pltpu.VMEM((TOTAL // LANES * PITCH, LANES), f32),
            pltpu.VMEM((2, 16, DEVICES, LANES), f32),
        ],
        compiler_params=PARAMS,
        name="dedisperse",
    )(chirp, fwd, bwd, end, tw, *coded)


def finish(coded):
    return pl.pallas_call(
        finish_kernel,
        grid=(16 // SUBS,),
        out_shape=(jax.ShapeDtypeStruct((4096, LANES), f32), jax.ShapeDtypeStruct((128, LANES), f32)),
        in_specs=[pl.BlockSpec((SUBS * STA * ROWS, LANES), lambda s: (s, 0))],
        out_specs=(
            pl.BlockSpec((SUBS * 256, LANES), lambda s: (s, 0)),
            pl.BlockSpec((128, LANES), lambda s: (0, 0)),
        ),
        compiler_params=PARAMS,
        name="finish",
    )(coded)


def exchange(blocks):
    received = [blocks[0]]
    for block, hop in zip(blocks[1:], HOPS[1:]):
        pairs = [(x * 4 + y, (x + hop[0]) % 2 * 4 + (y + hop[1]) % 4) for x in range(2) for y in range(4)]
        received.append(lax.ppermute(block, "sta", pairs))
    return received


def shards(voltages, beam_weights, station_delays, dm_index):
    blocks = shift(voltages, station_delays)
    chirp, left = chirps(dm_index.reshape(BEAMS), blocks[0], beam_weights)
    coded = exchange(beamform(exchange(blocks), left))
    coded = dedisperse(chirp, coded).reshape(DEVICES, 1, ROWS * LANES)
    coded = lax.all_to_all(coded, ("sub", "sta"), 0, 0, tiled=True).reshape(DEVICES * ROWS, LANES)
    moved, intensity = finish(coded)
    return moved.reshape(16, 2, 32, 1, 512), intensity.reshape(32, 1, 512)


def solution(mesh):
    return jax.shard_map(
        shards,
        mesh=mesh,
        in_specs=(
            P("sub", None, "sta", None),
            P("sub", None, None, None),
            P("sta"),
            P("sta", None),
        ),
        out_specs=(P(None, None, None, None, ("sub", "sta")), P(None, None, ("sub", "sta"))),
        check_vma=False,
    )
```

```python
import functools

import jax
import jax.numpy as jnp
import numpy as np
from jax import lax
from jax.experimental import pallas as pl
from jax.experimental.pallas import tpu as pltpu
from jax.sharding import PartitionSpec as P

TWO_PI = 6.283185307179586
DISPERSION = 4148808000.0
DM_STEP = 10.0
BASE_FREQ = 120.0
CHANNEL_WIDTH = 0.1953125

TOTAL = 65536
ROOT = 256
HALF = 128
LANES = 128
STA = 8
BLOCK = TOTAL // STA
TILES = BLOCK // LANES
BEAMS = 4
DEVICES = 128
ROWS = 17
CODE_STEP = 64.0
LEVELS = 32767.0
FLOOR = 1e-33

HOPS = [(0, 0), (1, 0), (0, 2), (1, 3), (0, 1), (1, 1), (0, 3), (1, 2)]


f32 = jnp.float32
bf16 = jnp.bfloat16


def neighbour(hop, sign):
    me = lax.axis_index("sta")
    x = (lax.shift_right_logical(me, 2) + hop[0]) & 1
    y = ((me & 3) + sign * hop[1]) & 3
    return x * 4 + y


def split_np(table):
    high = table.astype(bf16)
    low = (table - high.astype(np.float64)).astype(bf16)
    return high, low


@functools.lru_cache(maxsize=None)
def tables():
    m = np.arange(HALF)
    fwd = []
    for parity in range(2):
        angle = 2 * np.pi * (((2 * m[:, None] + parity) * m[None, :]) % ROOT) / ROOT
        c, s = np.cos(angle), np.sin(angle)
        fwd.append(np.block([[c, s], [-s, c]]))
    fwd = np.stack(fwd)
    bwd = fwd.transpose(0, 2, 1)
    order = (2 * np.arange(64)[None, :] + np.arange(2)[:, None]).reshape(-1)
    order = np.concatenate([order, HALF + order])
    last = bwd[:, order, :] / TOTAL

    def pair(t):
        return np.stack(split_np(t), axis=1)

    rows = np.concatenate([2 * m, 2 * m + 1])
    angle = 2 * np.pi * (rows[:, None] * np.arange(ROOT)[None, :]) / TOTAL
    twiddle = np.stack([np.cos(angle), np.sin(angle)]).astype(np.float32)
    return pair(fwd), pair(bwd), pair(last), twiddle


def code_of(peak):
    return jnp.ceil(jnp.log(jnp.maximum(peak, FLOOR)) * (CODE_STEP / 0.6931471805599453)) + 1.0


def scale_of(code):
    return jnp.exp2(code * (1.0 / CODE_STEP))


def quantize(x, inverse):
    return jnp.round(x * inverse).astype(jnp.int32).astype(jnp.int16)


def widen(q):
    return q.astype(jnp.int32).astype(f32)


PITCH = 9
FRONT = 136


def shift_kernel(delay_hbm, v_hbm, *refs):
    out_refs = refs[:STA]
    v_ref, delay_ref, plain_ref, turned_ref, sems = refs[STA:]
    halves_at = [pl.ds(h * (TOTAL // 2), TOTAL // 2) for h in range(2)]
    delays = pltpu.make_async_copy(delay_hbm, delay_ref, sems.at[4])
    delays.start()
    copies = []
    for p in range(2):
        for h in range(2):
            source, to = v_hbm.at[0, p, :, halves_at[h]], v_ref.at[p, :, halves_at[h]]
            copies.append(pltpu.make_async_copy(source, to, sems.at[p * 2 + h]))
            copies[-1].start()
    delays.wait()
    count = TOTAL // LANES
    lane = lax.broadcasted_iota(jnp.int32, (STA, LANES), 1)
    row = lax.broadcasted_iota(jnp.int32, (STA, LANES), 0)
    fine = jnp.zeros((STA, LANES), jnp.int32)
    for q in range(STA):
        fine = jnp.where(row == q, delay_ref[q] & (LANES - 1), fine)
    keep = lane >= fine
    source = lax.broadcasted_iota(jnp.int32, (LANES, LANES), 0)
    target = lax.broadcasted_iota(jnp.int32, (LANES, LANES), 1)
    turn = (target - source) & (LANES - 1)
    none = jnp.zeros((LANES, LANES), bf16)
    matrices = []
    for q in range(0, STA, 2):
        pair = [(turn == (delay_ref[q + i] & (LANES - 1))).astype(f32).astype(bf16) for i in range(2)]
        top = jnp.concatenate([pair[0], none], axis=1)
        low = jnp.concatenate([none, pair[1]], axis=1)
        matrices.append(jnp.concatenate([top, low], axis=0))
    unroll = 8
    rows = count + 8
    steps = count // unroll
    for p in range(2):
        plain = plain_ref.at[p]

        def fill(i, carry):
            at = pl.multiple_of(i * (unroll * LANES), unroll * LANES)
            x = v_ref[p, :, pl.ds(at, unroll * LANES)].astype(f32)
            for u in range(unroll):
                to = (FRONT + i * unroll + u) * PITCH
                plain[pl.ds(to, STA), :] = x[:, u * LANES : (u + 1) * LANES]
            return carry

        def wrap(i, carry):
            at = pl.multiple_of((TOTAL - FRONT * LANES) + i * (unroll * LANES), unroll * LANES)
            x = v_ref[p, :, pl.ds(at, unroll * LANES)].astype(f32)
            for u in range(unroll):
                to = (i * unroll + u) * PITCH
                plain[pl.ds(to, STA), :] = x[:, u * LANES : (u + 1) * LANES]
            return carry

        for h in range(2):
            copies[p * 2 + h].wait()
            lax.fori_loop(h * steps // 2, (h + 1) * steps // 2, fill, 0, unroll=4)
        lax.fori_loop(0, FRONT // unroll, wrap, 0, unroll=2)
    for q in range(0, STA, 2):
        for p in range(2):
            x = []
            for i in range(2):
                coarse = lax.shift_right_logical(delay_ref[q + i], 7)
                first = (FRONT - 8 - coarse) * PITCH + q + i
                x.append(plain_ref.at[p][pl.ds(first, rows, stride=PITCH), :].astype(bf16))
            y = jnp.dot(jnp.concatenate(x, axis=1), matrices[q // 2], preferred_element_type=f32)
            for i in range(2):
                turned_ref.at[p][pl.ds(q + i, rows, stride=PITCH), :] = y[:, i * LANES : (i + 1) * LANES]

    for out_ref, hop in zip(out_refs, HOPS):
        first = neighbour(hop, 1) * TILES

        def merge(i, before):
            at = pl.multiple_of(i * (unroll * LANES), unroll * LANES)
            last = []
            for p in range(2):
                parts = []
                old = before[p]
                for u in range(unroll):
                    tile = 8 + first + i * unroll + u
                    now = turned_ref[p, pl.ds(tile * PITCH, STA), :]
                    parts.append(jnp.where(keep, now, old))
                    old = now
                out_ref[p, :, pl.ds(at, unroll * LANES)] = jnp.concatenate(parts, axis=1).astype(bf16)
                last.append(old)
            return tuple(last)

        start = tuple(turned_ref[p, pl.ds((7 + first) * PITCH, STA), :] for p in range(2))
        lax.fori_loop(0, TILES // unroll, merge, start, unroll=4)


def beam_kernel(left_ref, *refs):
    v_refs, out_refs, sums_ref = refs[:STA], refs[STA : 2 * STA], refs[2 * STA]
    left = left_ref[...]
    chunk = 1024
    peak = jnp.zeros((64, LANES), f32)
    for i in range(BLOCK // chunk):
        at = slice(i * chunk, (i + 1) * chunk)
        volts = jnp.concatenate([v[0, :, at] for v in v_refs] + [v[1, :, at] for v in v_refs], axis=0)
        sums = jnp.dot(left, volts, preferred_element_type=f32)
        sums_ref[:, at] = sums
        for u in range(chunk // LANES):
            peak = jnp.maximum(peak, jnp.abs(sums[:, u * LANES : (u + 1) * LANES]))
    code = code_of(peak)
    inverse = LEVELS / scale_of(code)
    for d in range(STA):
        at8 = slice(d * 8, d * 8 + 8)
        factor = inverse[at8]
        out_ref = out_refs[d]
        out_ref[:, BLOCK:] = code[at8].astype(jnp.int32).astype(jnp.int16)

        def pack(i, carry):
            at = pl.multiple_of(i * 1024, 1024)
            x = sums_ref[at8, pl.ds(at, 1024)]
            x = x * jnp.concatenate([factor] * 8, axis=1)
            out_ref[:, pl.ds(at, 1024)] = jnp.round(x).astype(jnp.int32).astype(jnp.int16)
            return carry

        lax.fori_loop(0, BLOCK // 1024, pack, 0, unroll=4)


def halves(x, axis):
    high = x.astype(bf16)
    low = (x - high.astype(f32)).astype(bf16)
    return jnp.concatenate([high, low, high], axis=axis)


def dot_left(table_ref, parity, u):
    high, low = table_ref[parity, 0], table_ref[parity, 1]
    return jnp.dot(jnp.concatenate([high, high, low], axis=1), halves(u, 0), preferred_element_type=f32)


def dot_right(u, table_ref, parity):
    high, low = table_ref[parity, 0], table_ref[parity, 1]
    return jnp.dot(halves(u, 1), jnp.concatenate([high, high, low], axis=0), preferred_element_type=f32)


QUARTER_HIGH = 1.5703125
QUARTER_LOW = float(np.float32(np.pi / 2 - QUARTER_HIGH))


def cos_sin(phase):
    turns = jnp.round(phase * (2 / np.pi))
    r = (phase - turns * QUARTER_HIGH) - turns * QUARTER_LOW
    quadrant = turns.astype(jnp.int32)
    z = r * r
    s = r + r * z * (-1.6666654611e-1 + z * (8.3321608736e-3 + z * (-1.9515295891e-4)))
    c = 1.0 - 0.5 * z + z * z * (4.166664568298827e-2 + z * (-1.388731625493765e-3 + z * 2.443315711809948e-5))
    odd = (quadrant & 1) == 1
    cos = jnp.where(odd, s, c)
    sin = jnp.where(odd, c, s)
    cos = jnp.where(((quadrant + 1) & 2) == 2, -cos, cos)
    sin = jnp.where((quadrant & 2) == 2, -sin, sin)
    return cos, sin


def tables_kernel(dm_ref, after_ref, w_ref, out_ref, left_ref):
    w = w_ref[0].astype(f32)
    rows = []
    for d in range(STA):
        w_re = w[0, d * BEAMS : (d + 1) * BEAMS]
        w_im = w[1, d * BEAMS : (d + 1) * BEAMS]
        rows.append(jnp.concatenate([w_re, -w_im], axis=1))
        rows.append(jnp.concatenate([w_im, w_re], axis=1))
    left = jnp.concatenate(rows, axis=0).astype(bf16)
    old = lax.broadcasted_iota(jnp.int32, (128, 128), 0)
    new = lax.broadcasted_iota(jnp.int32, (128, 128), 1)
    group = lax.shift_right_logical(new, 3) & 7
    wanted = (new & 64) | (new & 7)
    for r, hop in enumerate(HOPS):
        wanted = jnp.where(group == r, wanted + neighbour(hop, -1) * 8, wanted)
    left = jnp.dot(left, (old == wanted).astype(f32).astype(bf16), preferred_element_type=f32).astype(bf16)
    new = lax.broadcasted_iota(jnp.int32, (64, 64), 0)
    old = lax.broadcasted_iota(jnp.int32, (64, 64), 1)
    group = lax.shift_right_logical(new, 3)
    wanted = new & 7
    for r, hop in enumerate(HOPS):
        wanted = jnp.where(group == r, wanted + neighbour(hop, 1) * 8, wanted)
    left = jnp.dot((old == wanted).astype(f32).astype(bf16), left, preferred_element_type=f32).astype(bf16)
    left_ref[...] = left
    centre = BASE_FREQ + CHANNEL_WIDTH * (lax.axis_index("sub").astype(f32) + 0.5)
    row = lax.broadcasted_iota(jnp.int32, (8, ROOT), 0)
    col = lax.broadcasted_iota(jnp.int32, (8, ROOT), 1)
    k2 = ROOT * (2 * (col & (HALF - 1)) + lax.shift_right_logical(col, 7))
    measures = [DM_STEP * dm_ref[b].astype(f32) for b in range(BEAMS)]

    def chirp(i, carry):
        at = pl.ds(pl.multiple_of(i * 8, 8), 8)
        k1 = 2 * ((row + i * 8) & (HALF - 1)) + i // (HALF // 8)
        position = k1 + k2
        signed = jnp.where(position < TOTAL // 2, position, position - TOTAL)
        offset = CHANNEL_WIDTH * signed.astype(f32) / TOTAL
        base = (TWO_PI * DISPERSION) * offset * offset / (centre * centre * (centre + offset))
        for b in range(BEAMS):
            c, s = cos_sin(measures[b] * base)
            out_ref[b, 0, at, :] = c
            out_ref[b, 1, at, :] = s
        return carry

    lax.fori_loop(0, ROOT // 8, chirp, 0, unroll=2)


def dedisperse_kernel(
    chirp_ref, fwd_ref, bwd_ref, end_ref, tw_ref, *refs
):
    x_refs, out_ref, time_ref, last_ref = refs[:STA], refs[STA], refs[STA + 1], refs[STA + 2]
    for x_ref, hop in zip(x_refs, HOPS):
        scale = scale_of(widen(x_ref[:, BLOCK:])) * (1.0 / LEVELS)
        first_tile = neighbour(hop, -1) * TILES

        def decode(i, carry):
            at = pl.multiple_of(i * 512, 512)
            x = widen(x_ref[:, pl.ds(at, 512)])
            for u in range(4):
                time_ref[pl.ds((first_tile + i * 4 + u) * PITCH, 8), :] = x[:, u * LANES : (u + 1) * LANES] * scale
            return carry

        lax.fori_loop(0, TILES // 4, decode, 0, unroll=4)

    def beam(b):
        x = []
        for p in range(2):
            x.append(
                jnp.concatenate([time_ref[pl.ds(h * PITCH + p * 4 + b, ROOT, stride=2 * PITCH), :] for h in range(2)], axis=1)
            )
        yield
        outs = []
        for parity in range(2):
            u = [v[:HALF] + v[HALF:] if parity == 0 else v[:HALF] - v[HALF:] for v in x]
            u = jnp.concatenate(u, axis=0)
            outs.append(dot_left(fwd_ref, parity, u))
        yield
        re = jnp.concatenate([o[:HALF] for o in outs], axis=0)
        im = jnp.concatenate([o[HALF:] for o in outs], axis=0)
        tw_re, tw_im = tw_ref[0], tw_ref[1]
        re, im = re * tw_re + im * tw_im, im * tw_re - re * tw_im
        outs = []
        for parity in range(2):
            u = [v[:, :HALF] + v[:, HALF:] if parity == 0 else v[:, :HALF] - v[:, HALF:] for v in (re, im)]
            u = jnp.concatenate(u, axis=1)
            outs.append(dot_right(u, bwd_ref, parity))
        yield
        sums = []
        for parity in range(2):
            at = slice(parity * HALF, (parity + 1) * HALF)
            c, s = chirp_ref[b, 0, :, at], chirp_ref[b, 1, :, at]
            y_re, y_im = outs[parity][:, :HALF], outs[parity][:, HALF:]
            u = jnp.concatenate([y_re * c - y_im * s, y_re * s + y_im * c], axis=1)
            sums.append(dot_right(u, fwd_ref, parity))
        yield
        top, bottom = sums[0] + sums[1], sums[0] - sums[1]
        re = jnp.concatenate([top[:, :HALF], bottom[:, :HALF]], axis=1)
        im = jnp.concatenate([top[:, HALF:], bottom[:, HALF:]], axis=1)
        re, im = re * tw_re - im * tw_im, im * tw_re + re * tw_im
        sums = []
        for parity in range(2):
            at = slice(parity * HALF, (parity + 1) * HALF)
            u = jnp.concatenate([re[at], im[at]], axis=0)
            sums.append(dot_left(end_ref, parity, u))
        yield
        top, bottom = sums[0] + sums[1], sums[0] - sums[1]
        for p in range(2):
            for r in range(2):
                at = slice(p * HALF + r * 64, p * HALF + r * 64 + 64)
                for h in range(2):
                    lanes = slice(h * LANES, (h + 1) * LANES)
                    first = b * 4 + r * 2 + h
                    last_ref[p, first, :64] = top[at, lanes]
                    last_ref[p, first, 64:] = bottom[at, lanes]

    running = [beam(b) for b in range(BEAMS)]
    for tick in range(6):
        for b in range(BEAMS):
            if tick >= 0 * b:
                next(running[b], None)

    def encode(i, carry):
        at = pl.ds(pl.multiple_of(i * 8, 8), 8)
        x = [[last_ref[p, k, at, :] for k in range(16)] for p in range(2)]
        peak = jnp.abs(x[0][0])
        for k in range(1, 32):
            peak = jnp.maximum(peak, jnp.abs(x[k // 16][k % 16]))
        code = code_of(peak)
        inverse = LEVELS / scale_of(code)
        first = i * (8 * ROWS)
        for k in range(16):
            low = jnp.round(x[0][k] * inverse).astype(jnp.int32) & 0xFFFF
            high = jnp.round(x[1][k] * inverse).astype(jnp.int32) << 16
            out_ref[pl.ds(first + k, 8, stride=ROWS), :] = low | high
        out_ref[pl.ds(first + 16, 8, stride=ROWS), :] = code.astype(jnp.int32)
        return carry

    lax.fori_loop(0, DEVICES // 8, encode, 0, unroll=4)


SUBS = 4


def finish_kernel(x_ref, out_ref, power_ref):
    step = pl.program_id(0)

    @pl.when(step == 0)
    def _():
        power_ref[...] = jnp.zeros_like(power_ref)

    scales = []
    for sub in range(SUBS):
        code = x_ref[pl.ds(sub * STA * ROWS + 16, STA, stride=ROWS), :]
        scales.append(scale_of(code.astype(f32)) * (1.0 / LEVELS))
    for sta in range(STA):
        power = power_ref[sta * 16 : sta * 16 + 16, :]
        for sub in range(SUBS):
            src = (sub * STA + sta) * ROWS
            to = sub * 256 + sta * 16
            scale = jnp.broadcast_to(scales[sub][sta : sta + 1], (16, LANES))
            both = x_ref[src : src + 16, :]
            re = ((both << 16) >> 16).astype(f32) * scale
            im = (both >> 16).astype(f32) * scale
            out_ref[to : to + 16, :] = re
            out_ref[to + 128 : to + 144, :] = im
            power = power + (re * re + im * im)
        power_ref[sta * 16 : sta * 16 + 16, :] = power

    @pl.when(step == pl.num_programs(0) - 1)
    def _():
        power_ref[...] = power_ref[...] * (1.0 / 16.0)


VMEM = pl.BlockSpec(memory_space=pltpu.VMEM)
SMEM = pl.BlockSpec(memory_space=pltpu.SMEM)
HBM = pl.BlockSpec(memory_space=pltpu.HBM)
PARAMS = pltpu.CompilerParams(vmem_limit_bytes=36 * 1024 * 1024)


SHIFT_PARAMS = pltpu.CompilerParams(vmem_limit_bytes=50 * 1024 * 1024 + 512 * 1024)


def shift(voltages, delays):
    return pl.pallas_call(
        shift_kernel,
        out_shape=[jax.ShapeDtypeStruct((2, STA, BLOCK), bf16)] * STA,
        in_specs=[HBM, HBM],
        out_specs=[VMEM] * STA,
        scratch_shapes=[
            pltpu.VMEM((2, STA, TOTAL), bf16),
            pltpu.SMEM((STA,), jnp.int32),
            pltpu.VMEM((2, (TOTAL // LANES + FRONT) * PITCH, LANES), f32),
            pltpu.VMEM((2, (TOTAL // LANES + 8) * PITCH, LANES), f32),
            pltpu.SemaphoreType.DMA((5,)),
        ],
        compiler_params=SHIFT_PARAMS,
        name="shift",
    )(delays, voltages)


def beamform(volts, left):
    return pl.pallas_call(
        beam_kernel,
        out_shape=[jax.ShapeDtypeStruct((8, BLOCK + LANES), jnp.int16)] * STA,
        in_specs=[VMEM] * (1 + STA),
        out_specs=[VMEM] * STA,
        scratch_shapes=[pltpu.VMEM((64, BLOCK), f32)],
        compiler_params=PARAMS,
        name="beamform",
    )(left, *volts)


def chirps(dm_index, after, weights):
    return pl.pallas_call(
        tables_kernel,
        out_shape=(
            jax.ShapeDtypeStruct((BEAMS, 2, ROOT, ROOT), f32),
            jax.ShapeDtypeStruct((64, 128), bf16),
        ),
        in_specs=[SMEM, HBM, VMEM],
        out_specs=(VMEM, VMEM),
        compiler_params=PARAMS,
        cost_estimate=pl.CostEstimate(flops=20_000_000, transcendentals=0, bytes_accessed=2 << 20),
        name="chirps",
    )(dm_index, after, weights)


def dedisperse(chirp, coded):
    fwd, bwd, end, tw = tables()
    return pl.pallas_call(
        dedisperse_kernel,
        out_shape=jax.ShapeDtypeStruct((DEVICES * ROWS, LANES), jnp.int32),
        in_specs=[VMEM] * (5 + STA),
        out_specs=VMEM,
        scratch_shapes=[
            pltpu.VMEM((TOTAL // LANES * PITCH, LANES), f32),
            pltpu.VMEM((2, 16, DEVICES, LANES), f32),
        ],
        compiler_params=PARAMS,
        name="dedisperse",
    )(chirp, fwd, bwd, end, tw, *coded)


def finish(coded):
    return pl.pallas_call(
        finish_kernel,
        grid=(16 // SUBS,),
        out_shape=(jax.ShapeDtypeStruct((4096, LANES), f32), jax.ShapeDtypeStruct((128, LANES), f32)),
        in_specs=[pl.BlockSpec((SUBS * STA * ROWS, LANES), lambda s: (s, 0))],
        out_specs=(
            pl.BlockSpec((SUBS * 256, LANES), lambda s: (s, 0)),
            pl.BlockSpec((128, LANES), lambda s: (0, 0)),
        ),
        compiler_params=PARAMS,
        name="finish",
    )(coded)


def exchange(blocks):
    received = [blocks[0]]
    for block, hop in zip(blocks[1:], HOPS[1:]):
        pairs = [(x * 4 + y, (x + hop[0]) % 2 * 4 + (y + hop[1]) % 4) for x in range(2) for y in range(4)]
        received.append(lax.ppermute(block, "sta", pairs))
    return received


def shards(voltages, beam_weights, station_delays, dm_index):
    blocks = shift(voltages, station_delays)
    chirp, left = chirps(dm_index.reshape(BEAMS), blocks[0], beam_weights)
    coded = exchange(beamform(exchange(blocks), left))
    coded = dedisperse(chirp, coded).reshape(DEVICES, 1, ROWS * LANES)
    coded = lax.all_to_all(coded, ("sub", "sta"), 0, 0, tiled=True).reshape(DEVICES * ROWS, LANES)
    moved, intensity = finish(coded)
    return moved.reshape(16, 2, 32, 1, 512), intensity.reshape(32, 1, 512)


def solution(mesh):
    return jax.shard_map(
        shards,
        mesh=mesh,
        in_specs=(
            P("sub", None, "sta", None),
            P("sub", None, None, None),
            P("sta"),
            P("sta", None),
        ),
        out_specs=(P(None, None, None, None, ("sub", "sta")), P(None, None, ("sub", "sta"))),
        check_vma=False,
    )
```
